512 devices in a mesh: tok: 64 (over y, z), tp: 8 (over x, core).
Axes of the slice: x: 4, y: 8, z: 8, core: 2. Of those that a mesh axis runs over, the one named last changes fastest.
Arguments:
- hidden: bfloat16 [6144, 8192], P('tok'), may hold values from -2600 to 2600
- norm_gain: float32 [8192], replicated, may hold values from 0.5 to 1.5
- w_query: bfloat16 [8192, 4096], P('tok', 'tp'), may hold values from -1 to 1
- w_key: bfloat16 [8192, 1024], P('tok', 'tp'), may hold values from -1 to 1
- w_value: bfloat16 [8192, 1024], P('tok', 'tp'), may hold values from -0.0625 to 0.0625
- doc_ids: int32 [6144], P('tok'), may hold values from 0 to 3, as said below
Outputs:
- attended: bfloat16 [6144, 4096], P('tok', 'tp')
- out_scale: float32 [4096], P('tp')
- folded_gain: float32 [8192], P(('tok', 'tp'))
- codes_query: float32 [8192, 4096], P(('tok', 'tp'))
- codes_key: float32 [8192, 1024], P(('tok', 'tp'))
- codes_value: float32 [8192, 1024], P(('tok', 'tp'))
- scale_query: float32 [4096], P('tp')
- scale_key: float32 [1024], P('tp')
- scale_value: float32 [1024], P('tp')
The draws below stay inside these ranges and needn't reach their ends.
Inputs may be any that keep to these rules, and one draw needn't show every extreme that they name: doc_ids never falls along the tokens; each of the 4 documents holds 1 to 4608 tokens and one holds exactly 4608.
All inputs are finite; a program needn't handle non-finite values. Where the reference program divides by a largest or mean magnitude, that divisor is 1e-20 or more.
Results may differ from the reference program's by a relative error of at most 0.005.
The reference program's roundings to bfloat16 on the way (of `normed` and `value`) count: a program that leaves them out, or rounds other values in their place, can miss the bound.
Values may be sent and summed in bfloat16 or wider, within the bound.
No kernel may reach another device: no remote copies, remote signals or barrier semaphores. Data moves between devices by JAX's collectives and lax.ppermute only.
A program may use at most 64 MiB of HBM per device.

```python
import math
import jax
import jax.numpy as jnp
from jax import lax

D = 8192
HEAD = 128
KVH = 8
QHEADS = 32
DOCS = 4
TOKENS = 6144
DOC_MOST = 4608


pair_count = 6


strengths = (0.75, 0.55, 0.35, 0.75, 0.55, 0.35)


planted_entry = 1.0


def document_layout(key):
    folded = jax.random.fold_in(key, 5151)
    key_where, key_cuts = jax.random.split(folded, 2)
    short_total = TOKENS - DOC_MOST
    long_place = jax.random.randint(key_where, (), 0, DOCS)
    cut_order = jax.random.permutation(key_cuts, short_total - 1)[:DOCS - 2] + 1
    cuts = jnp.sort(cut_order)
    bounds = jnp.concatenate([jnp.zeros((1,), jnp.int32), cuts.astype(jnp.int32), jnp.full((1,), short_total, jnp.int32)])
    shorts = bounds[1:] - bounds[:-1]
    order = jnp.arange(DOCS, dtype=jnp.int32)
    short_index = jnp.clip(order - (order > long_place).astype(jnp.int32), 0, DOCS - 2)
    lengths = jnp.where(order == long_place, DOC_MOST, shorts[short_index]).astype(jnp.int32)
    ends = jnp.cumsum(lengths).astype(jnp.int32)
    long_start = ends[long_place] - DOC_MOST
    return (ends, long_start)


def planted_layout(key):
    folded = jax.random.fold_in(key, 4242)
    key_perm, key_place, key_sign = jax.random.split(folded, 3)
    channels = jax.random.permutation(key_perm, D)[:3 * pair_count]
    ends, long_start = document_layout(key)
    stride = TOKENS // 4 // pair_count
    offsets = jax.random.randint(key_place, (pair_count,), 1, stride)
    later = long_start + TOKENS // 2 + jnp.arange(pair_count, dtype=jnp.int32) * stride + offsets
    reach = jnp.where(jnp.arange(pair_count) % 2 == 0, TOKENS // 2, 1)
    earlier = later - reach
    signs = jnp.where(jax.random.bernoulli(key_sign, 0.5, (KVH, HEAD)), 1.0, -1.0)
    half_head = HEAD // 2
    band_size = max(HEAD // 32, 2)
    band_start = half_head - band_size
    within = jnp.arange(HEAD) % half_head
    band = ((within >= band_start) & (within < band_start + band_size)).astype(jnp.float32)
    return (channels, later, earlier, signs * band[None, :])


def draw_doc_ids(key, part):
    ends, long_start = document_layout(key)
    token_index = jnp.arange(TOKENS, dtype=jnp.int32)
    return jnp.sum((token_index[:, None] >= ends[None, :DOCS - 1]).astype(jnp.int32), axis=1).astype(jnp.int32)


def main_rows(channels):
    row_index = jnp.arange(D)[:, None]
    is_main = jnp.any(row_index == channels[None, :pair_count], axis=1)
    is_extra = jnp.any(row_index == channels[None, pair_count:], axis=1)
    return (is_main, is_extra)


def drawn_weight(key, salt, columns):
    values = jnp.clip(jax.random.normal(jax.random.fold_in(key, salt), (D, columns), jnp.float32), -4.0, 4.0) / math.sqrt(D)
    return jnp.clip(values, -planted_entry, planted_entry)


def draw_w_query(key, part):
    values = drawn_weight(key, 11, QHEADS * HEAD)
    channels, later, earlier, pattern = planted_layout(key)
    is_main, is_extra = main_rows(channels)
    pattern_row = jnp.repeat(pattern, QHEADS // KVH, axis=0).reshape(QHEADS * HEAD)
    values = jnp.where(is_main[:, None], pattern_row[None, :], jnp.where(is_extra[:, None], 0.0, values))
    return values.astype(jnp.bfloat16)


def draw_w_key(key, part):
    values = drawn_weight(key, 12, KVH * HEAD)
    channels, later, earlier, pattern = planted_layout(key)
    is_main, is_extra = main_rows(channels)
    pattern_row = pattern.reshape(KVH * HEAD)
    values = jnp.where(is_main[:, None], pattern_row[None, :], jnp.where(is_extra[:, None], 0.0, values))
    return values.astype(jnp.bfloat16)


def draw_norm_gain(key, part):
    key_gain = jax.random.fold_in(key, 31)
    channels, later, earlier, pattern = planted_layout(key)
    is_main, is_extra = main_rows(channels)
    nearby = jax.random.uniform(jax.random.fold_in(key, 32), (D,), jnp.float32, 0.95, 1.05)
    spread = 1.0 + 0.1 * jnp.clip(jax.random.normal(key_gain, (D,), jnp.float32), -5.0, 5.0)
    return jnp.where(is_main, nearby, spread)


def draw_hidden(key, part):
    key_base, key_channel = jax.random.split(key, 2)
    base = jnp.clip(jax.random.normal(key_base, (TOKENS, D), jnp.float32), -4.0, 4.0)
    channels, later, earlier, pattern = planted_layout(key)
    column_index = jnp.arange(D)[None, :]
    main_hot = (column_index == channels[:pair_count, None]).astype(jnp.float32)
    is_main_column = jnp.sum(main_hot, axis=0, keepdims=True) > 0.5
    channel = jnp.exp(jax.random.uniform(key_channel, (1, D), jnp.float32, 0.0, math.log(30.0)))
    channel = jnp.where(is_main_column, 1.0, channel)
    values = base * channel
    token_index = jnp.arange(TOKENS)[:, None]
    is_later = (token_index == later[None, :]).astype(jnp.float32)
    is_earlier = (token_index == earlier[None, :]).astype(jnp.float32)
    late_hot = (column_index == channels[pair_count:2 * pair_count, None]).astype(jnp.float32)
    early_hot = (column_index == channels[2 * pair_count:, None]).astype(jnp.float32)
    levels = jnp.array(strengths, jnp.float32)
    main_amp = jnp.sqrt(levels)[:, None]
    rest_amp = jnp.sqrt(1.0 - levels - 0.0025)[:, None]
    late_rows = main_amp * main_hot + rest_amp * late_hot
    early_rows = main_amp * main_hot + rest_amp * early_hot
    planted = math.sqrt(D) * (jnp.dot(is_later, late_rows, precision=lax.Precision.HIGHEST) + jnp.dot(is_earlier, early_rows, precision=lax.Precision.HIGHEST))
    chosen = jnp.sum(is_later + is_earlier, axis=1) > 0.5
    values = jnp.where(chosen[:, None], 0.05 * base + planted, values)
    return jnp.clip(values, -2600.0, 2600.0).astype(jnp.bfloat16)


def block_levels(key, shape, shards, smallest, top_value):
    def one(position, shards_of):
        heights = jax.random.uniform(jax.random.fold_in(jax.random.fold_in(key, 6), position), (shards_of,), jnp.float32, smallest / len(shards), top_value / len(shards))
        return jnp.repeat(jnp.exp(heights), shape[position] // shards_of).reshape((-1,) + (1,) * (len(shape) - position - 1))

    factor_of = one(*shards[0])
    for cut in shards[1:]:
        factor_of = factor_of * one(*cut)
    return factor_of


def normal_values(stream_key, shape, width, limit, shards=(), kind=jnp.bfloat16):
    values = jax.random.normal(stream_key, shape, jnp.float32) * width
    if len(shards) > 0:
        values = block_levels(stream_key, shape, shards, -0.22, 0.18) * values
    return jnp.clip(values, min=-limit, max=limit).astype(kind)


def setup_inputs(seed: int = 0) -> dict:
    key_list = jax.random.split(jax.random.key(seed), 7)
    hidden = draw_hidden(jax.random.fold_in(key_list[6], 71), 0)
    norm_gain = draw_norm_gain(jax.random.fold_in(key_list[6], 71), 0)
    w_query = draw_w_query(jax.random.fold_in(key_list[6], 71), 0)
    w_key = draw_w_key(jax.random.fold_in(key_list[6], 71), 0)
    w_value = normal_values(key_list[4], (D, KVH * HEAD), D ** -0.5, 0.0625, ((0, 64), (1, 8)))
    doc_ids = draw_doc_ids(jax.random.fold_in(key_list[6], 71), 0)
    return dict(hidden=hidden, norm_gain=norm_gain, w_query=w_query, w_key=w_key, w_value=w_value, doc_ids=doc_ids)


def rotate(states, positions):
    half = states.shape[-1] // 2
    inverse = jnp.exp(jnp.arange(half, dtype=jnp.float32) * (-2.0 * math.log(10000.0) / states.shape[-1]))
    angles = positions[:, None] * inverse[None, :]
    cosine = jnp.cos(angles)[:, None, :]
    sine = jnp.sin(angles)[:, None, :]
    first = states[..., :half]
    second = states[..., half:]
    return jnp.concatenate([first * cosine - second * sine, second * cosine + first * sine], axis=-1)

def quantize(smoothing, matrix):
    smoothed = smoothing[:, None] * matrix.astype(jnp.float32)
    column_scale = jnp.maximum(lax.optimization_barrier(jnp.max(jnp.abs(smoothed), axis=0)), 1e-05) / 127.0
    return (smoothed / column_scale[None, :], column_scale)

def reference(hidden, norm_gain, w_query, w_key, w_value, doc_ids):
    tokens = hidden.shape[0]
    states = hidden.astype(jnp.float32)
    normed = (states * lax.rsqrt(lax.optimization_barrier(jnp.mean(states * states, axis=1, keepdims=True)) + 1e-05) * norm_gain[None, :]).astype(jnp.bfloat16)
    input_peak = lax.optimization_barrier(jnp.max(jnp.abs(normed.astype(jnp.float32)), axis=0))
    positions = jnp.arange(tokens, dtype=jnp.float32)
    query = rotate(jnp.dot(normed, w_query, preferred_element_type=jnp.float32).reshape(tokens, QHEADS, HEAD), positions).astype(jnp.bfloat16)
    key = rotate(jnp.dot(normed, w_key, preferred_element_type=jnp.float32).reshape(tokens, KVH, HEAD), positions).astype(jnp.bfloat16)
    value = jnp.dot(normed, w_value, preferred_element_type=jnp.float32).astype(jnp.bfloat16).reshape(tokens, KVH, HEAD)
    group_size = QHEADS // KVH
    index = jnp.arange(tokens, dtype=jnp.int32)
    allowed = (doc_ids[:, None] == doc_ids[None, :]) & (index[None, :] <= index[:, None])
    score_scale = 1.0 / math.sqrt(HEAD)

    def one_head(head_index):
        query_head = lax.dynamic_index_in_dim(query, head_index, 1, keepdims=False)
        key_head = lax.dynamic_index_in_dim(key, head_index // group_size, 1, keepdims=False)
        value_head = lax.dynamic_index_in_dim(value, head_index // group_size, 1, keepdims=False)
        scores = jnp.dot(query_head, key_head.T, preferred_element_type=jnp.float32) * score_scale
        scores = jnp.where(allowed, scores, -1e+30)
        highest = lax.optimization_barrier(jnp.max(scores, axis=1, keepdims=True))
        weights = jnp.where(allowed, jnp.exp(scores - highest), 0.0)
        totals = lax.optimization_barrier(jnp.sum(weights, axis=1, keepdims=True))
        return jnp.dot(weights.astype(jnp.bfloat16), value_head, preferred_element_type=jnp.float32) / totals
    heads = lax.map(one_head, jnp.arange(QHEADS, dtype=jnp.int32))
    attended = heads.transpose(1, 0, 2).reshape(tokens, QHEADS * HEAD).astype(jnp.bfloat16)
    out_scale = lax.optimization_barrier(jnp.max(jnp.abs(attended.astype(jnp.float32)), axis=0))
    weight_peak = jnp.maximum(jnp.maximum(lax.optimization_barrier(jnp.max(jnp.abs(w_query.astype(jnp.float32)), axis=1)), lax.optimization_barrier(jnp.max(jnp.abs(w_key.astype(jnp.float32)), axis=1))), lax.optimization_barrier(jnp.max(jnp.abs(w_value.astype(jnp.float32)), axis=1)))
    smoothing = jnp.sqrt(jnp.maximum(input_peak, 1e-05)) / jnp.sqrt(jnp.maximum(weight_peak, 1e-05))
    folded_gain = norm_gain / smoothing
    codes_query, scale_query = quantize(smoothing, w_query)
    codes_key, scale_key = quantize(smoothing, w_key)
    codes_value, scale_value = quantize(smoothing, w_value)
    return (attended, out_scale, folded_gain, codes_query, codes_key, codes_value, scale_query, scale_key, scale_value)
```

```python
import math

import jax
import jax.numpy as jnp
from jax import lax
from jax.sharding import Mesh
from jax.sharding import PartitionSpec as P

HEAD = 128
KVH = 8
QHEADS = 32
TOK = ("tok_0", "tok_1")
TOK_TP = ("tok_0", "tok_1", "tp")


def exchange(parts, axis):
    return lax.all_to_all(parts, axis, split_axis=0, concat_axis=0, tiled=True)


def to_everyone(shard, axis):
    return exchange(jnp.broadcast_to(shard, (lax.axis_size(axis), *shard.shape)), axis)


def rotate(states, positions):
    half = states.shape[-1] // 2
    inverse = jnp.exp(
        jnp.arange(half, dtype=jnp.float32) * (-2.0 * math.log(10000.0) / states.shape[-1])
    )
    angles = positions[:, None] * inverse[None, :]
    cosine = jnp.cos(angles)[:, None, :]
    sine = jnp.sin(angles)[:, None, :]
    first = states[..., :half]
    second = states[..., half:]
    return jnp.concatenate(
        [first * cosine - second * sine, second * cosine + first * sine], axis=-1
    )


def smooth_from(input_peak, weight_peak):
    return jnp.sqrt(jnp.maximum(input_peak, 1e-05)) / jnp.sqrt(jnp.maximum(weight_peak, 1e-05))


def on_device(hidden, norm_gain, w_query, w_key, w_value, doc_ids):
    tok_dev, width = hidden.shape
    row_count = w_query.shape[0]
    tok_count = lax.axis_size(TOK)
    tp_count = lax.axis_size("tp")
    tok_index = lax.axis_index(TOK)
    tp_index = lax.axis_index("tp")
    sub_rows = row_count // tp_count
    widths = (w_query.shape[1], w_key.shape[1], w_value.shape[1])
    cuts = (widths[0], widths[0] + widths[1])
    columns = sum(widths)
    heads_here = widths[0] // HEAD
    kv_here = widths[1] // HEAD
    group_size = QHEADS // KVH

    block = jnp.concatenate((w_query, w_key, w_value), axis=1)
    gathered = lax.all_gather(block, TOK, axis=0, tiled=True)

    states = hidden.astype(jnp.float32)
    inverse_rms = lax.rsqrt(jnp.mean(states * states, axis=1, keepdims=True) + 1e-05)
    normed = (states * inverse_rms * norm_gain[None, :]).astype(jnp.bfloat16)

    peaks = jnp.max(jnp.abs(normed), axis=0).reshape(tok_count, row_count)
    docs = jnp.broadcast_to(doc_ids.astype(jnp.bfloat16), (tok_count, tok_dev))
    arrived = exchange(jnp.concatenate((peaks, docs), axis=1), TOK)
    input_peak = jnp.max(arrived[:, :row_count], axis=0).astype(jnp.float32)
    doc_block = arrived[:, row_count:].astype(jnp.int32).reshape(tok_count * tok_dev)

    row_peak = jnp.max(jnp.abs(block), axis=1)
    sent = jnp.concatenate(
        (
            block.reshape(tp_count, sub_rows * columns),
            jnp.broadcast_to(row_peak, (tp_count, row_count)),
        ),
        axis=1,
    )
    rows = exchange(sent, "tp")
    weight_peak = jnp.max(rows[:, sub_rows * columns :], axis=0).astype(jnp.float32)
    own_rows = rows[:, : sub_rows * columns].reshape(tp_count, sub_rows, columns)

    smoothing = smooth_from(input_peak, weight_peak)
    column_peak = jnp.max(jnp.abs(smoothing[:, None] * block.astype(jnp.float32)), axis=0)
    column_peak = jnp.max(to_everyone(column_peak, TOK), axis=0)
    scale = jnp.maximum(column_peak, 1e-05) / 127.0
    all_scales = to_everyone(scale, "tp")
    scales = jnp.split(scale, cuts)

    smooth_part = lax.dynamic_slice_in_dim(smoothing, tp_index * sub_rows, sub_rows)
    gain_part = lax.dynamic_slice_in_dim(
        norm_gain, tok_index * row_count + tp_index * sub_rows, sub_rows
    )
    folded_gain = gain_part / smooth_part
    coded = (
        smooth_part[None, :, None] * own_rows.astype(jnp.float32) / all_scales[:, None, :]
    )
    codes = tuple(
        part.transpose(1, 0, 2).reshape(sub_rows, tp_count * part.shape[2])
        for part in jnp.split(coded, cuts, axis=2)
    )

    held_gain = jnp.where(all_scales[0, 0] > 0.0, norm_gain, 0.0)
    held = (states * inverse_rms * held_gain[None, :]).astype(jnp.bfloat16)
    projected = jnp.split(
        jnp.dot(held, gathered, preferred_element_type=jnp.float32), cuts, axis=1
    )
    query_positions = tok_index * tok_dev + jnp.arange(tok_dev, dtype=jnp.int32)
    positions = query_positions.astype(jnp.float32)
    query = (
        rotate(projected[0].reshape(tok_dev, heads_here, HEAD), positions)
        .astype(jnp.bfloat16)
        .reshape(tok_dev, kv_here, group_size, HEAD)
    )
    key = (
        rotate(projected[1].reshape(tok_dev, kv_here, HEAD), positions)
        .astype(jnp.bfloat16)
        .reshape(tok_dev, kv_here * HEAD)
    )
    value = projected[2].astype(jnp.bfloat16)

    both = jnp.concatenate((key, value), axis=1)
    line = to_everyone(both, "tok_1").reshape(-1, both.shape[1])
    everything = lax.all_gather(line, "tok_0", axis=0, tiled=True)
    key_block, value_block = jnp.split(everything, (widths[1],), axis=1)

    length = key_block.shape[0]
    scores = jnp.einsum(
        "tkgd,skd->kgts",
        query,
        key_block.reshape(length, kv_here, HEAD),
        preferred_element_type=jnp.float32,
    ) * (1.0 / math.sqrt(HEAD))
    key_positions = jnp.arange(length, dtype=jnp.int32)
    allowed = (doc_ids[:, None] == doc_block[None, :]) & (
        key_positions[None, :] <= query_positions[:, None]
    )
    scores = jnp.where(allowed, scores, -1e30)
    highest = jnp.max(scores, axis=3, keepdims=True)
    weights = jnp.where(allowed, jnp.exp(scores - highest), 0.0)
    totals = jnp.sum(weights, axis=3)
    accumulated = jnp.einsum(
        "kgts,skd->kgtd",
        weights.astype(jnp.bfloat16),
        value_block.reshape(length, kv_here, HEAD),
        preferred_element_type=jnp.float32,
    )
    attended = (
        (accumulated / totals[..., None])
        .transpose(2, 0, 1, 3)
        .reshape(tok_dev, heads_here * HEAD)
        .astype(jnp.bfloat16)
    )
    out_peak = to_everyone(jnp.max(jnp.abs(attended), axis=0), TOK)
    out_scale = jnp.max(out_peak, axis=0).astype(jnp.float32)
    return (
        attended,
        out_scale,
        folded_gain,
        codes[0],
        codes[1],
        codes[2],
        scales[0],
        scales[1],
        scales[2],
    )


def solution(mesh):
    split = Mesh(mesh.devices.reshape(8, 8, mesh.shape["tp"]), ("tok_0", "tok_1", "tp"))
    placed = (P(TOK, None), P(), P(TOK, "tp"), P(TOK, "tp"), P(TOK, "tp"), P(TOK))
    return jax.shard_map(
        on_device,
        mesh=split,
        in_specs=placed,
        out_specs=(
            P(TOK, "tp"),
            P("tp"),
            P(TOK_TP),
            P(TOK_TP, None),
            P(TOK_TP, None),
            P(TOK_TP, None),
            P("tp"),
            P("tp"),
            P("tp"),
        ),
        check_vma=False,
    )
```

```python
import math

import jax
import jax.numpy as jnp
from jax import lax
from jax.sharding import Mesh
from jax.sharding import PartitionSpec as P

HEAD = 128
KVH = 8
QHEADS = 32
LINE = ("z", "pair")
TOK = ("y", "z", "pair")
TP = ("x", "core")
TOK_TP = TOK + TP


def exchange(parts, axis):
    return lax.all_to_all(parts, axis, split_axis=0, concat_axis=0, tiled=True)


def to_everyone(shard, axis):
    return exchange(jnp.broadcast_to(shard, (lax.axis_size(axis), *shard.shape)), axis)


def rotate(states, positions):
    half = states.shape[-1] // 2
    inverse = jnp.exp(
        jnp.arange(half, dtype=jnp.float32) * (-2.0 * math.log(10000.0) / states.shape[-1])
    )
    angles = positions[:, None] * inverse[None, :]
    cosine = jnp.cos(angles)[:, None, :]
    sine = jnp.sin(angles)[:, None, :]
    first = states[..., :half]
    second = states[..., half:]
    return jnp.concatenate(
        [first * cosine - second * sine, second * cosine + first * sine], axis=-1
    )


def smooth_from(input_peak, weight_peak):
    return jnp.sqrt(jnp.maximum(input_peak, 1e-05)) / jnp.sqrt(jnp.maximum(weight_peak, 1e-05))


def on_device(hidden, norm_gain, w_query, w_key, w_value, doc_ids):
    tok_dev, width = hidden.shape
    row_count = w_query.shape[0]
    tok_count = lax.axis_size(TOK)
    tp_count = lax.axis_size(TP)
    tok_index = lax.axis_index(TOK)
    tp_index = lax.axis_index(TP)
    side = lax.axis_index("pair")
    core = lax.axis_index("core")
    line = lax.axis_size("z") * 2
    sub_rows = row_count // tp_count
    widths = (w_query.shape[1], w_key.shape[1], w_value.shape[1])
    cuts = (widths[0], widths[0] + widths[1])
    columns = sum(widths)
    half_query = widths[0] // 2
    half_columns = half_query + HEAD
    heads_half = half_query // HEAD
    group_size = QHEADS // KVH

    halves = jnp.stack(
        (
            jnp.concatenate((w_query[:, :half_query], w_key), axis=1),
            jnp.concatenate((w_query[:, half_query:], w_value), axis=1),
        )
    )
    sent = jnp.broadcast_to(halves, (line // 2, *halves.shape))
    along_z = exchange(sent.reshape(line, row_count, half_columns), LINE)
    gathered = lax.all_gather(
        along_z.reshape(line * row_count, half_columns), "y", axis=0, tiled=True
    )

    states = hidden.astype(jnp.float32)
    inverse_rms = lax.rsqrt(jnp.mean(states * states, axis=1, keepdims=True) + 1e-05)
    normed = (states * inverse_rms * norm_gain[None, :]).astype(jnp.bfloat16)

    swap = [(0, 1), (1, 0)]
    channels = width // 2
    near = lax.ppermute(
        lax.dynamic_slice_in_dim(normed, core * channels, channels, axis=1), "pair", swap
    )
    far = lax.ppermute(near, "core", swap)
    other = jnp.concatenate(
        (jnp.where(core == 0, near, far), jnp.where(core == 0, far, near)), axis=1
    )

    peaks = jnp.max(jnp.abs(normed), axis=0).reshape(tok_count, row_count)
    docs = jnp.broadcast_to(doc_ids.astype(jnp.bfloat16), (tok_count, tok_dev))
    arrived = exchange(jnp.concatenate((peaks, docs), axis=1), TOK)
    input_peak = jnp.max(arrived[:, :row_count], axis=0).astype(jnp.float32)
    doc_block = arrived[:, row_count:].astype(jnp.int32).reshape(tok_count * tok_dev)

    block = jnp.concatenate((w_query, w_key, w_value), axis=1)
    row_peak = jnp.max(jnp.abs(block), axis=1)
    sent = jnp.concatenate(
        (
            block.reshape(tp_count, sub_rows * columns),
            jnp.broadcast_to(row_peak, (tp_count, row_count)),
        ),
        axis=1,
    )
    rows = exchange(sent, TP)
    weight_peak = jnp.max(rows[:, sub_rows * columns :], axis=0).astype(jnp.float32)
    own_rows = rows[:, : sub_rows * columns].reshape(tp_count, sub_rows, columns)

    smoothing = smooth_from(input_peak, weight_peak)
    column_peak = jnp.max(jnp.abs(smoothing[:, None] * block.astype(jnp.float32)), axis=0)
    column_peak = jnp.max(to_everyone(column_peak, TOK), axis=0)
    scale = jnp.maximum(column_peak, 1e-05) / 127.0
    all_scales = to_everyone(scale, TP)
    scales = jnp.split(scale, cuts)

    smooth_part = lax.dynamic_slice_in_dim(smoothing, tp_index * sub_rows, sub_rows)
    gain_part = lax.dynamic_slice_in_dim(
        norm_gain, tok_index * row_count + tp_index * sub_rows, sub_rows
    )
    folded_gain = gain_part / smooth_part
    coded = (
        smooth_part[None, :, None] * own_rows.astype(jnp.float32) / all_scales[:, None, :]
    )
    codes = tuple(
        part.transpose(1, 0, 2).reshape(sub_rows, tp_count * part.shape[2])
        for part in jnp.split(coded, cuts, axis=2)
    )

    even = (side == 0) & (all_scales[0, 0] > 0.0)
    both_rows = jnp.concatenate(
        (jnp.where(even, normed, other), jnp.where(even, other, normed)), axis=0
    )
    projected = jnp.dot(both_rows, gathered, preferred_element_type=jnp.float32)
    pair_positions = (tok_index - side) * tok_dev + jnp.arange(2 * tok_dev, dtype=jnp.int32)
    last = projected[:, half_query:]
    turned = rotate(
        projected.reshape(2 * tok_dev, heads_half + 1, HEAD), pair_positions.astype(jnp.float32)
    )
    kept = jnp.where(side == 0, turned[:, heads_half], last).astype(jnp.bfloat16)

    spread = to_everyone(kept, LINE).reshape(line // 2, 2, 2 * tok_dev, HEAD)
    spread = jnp.concatenate(
        (spread[:, 0].reshape(-1, HEAD), spread[:, 1].reshape(-1, HEAD)), axis=1
    )
    everything = lax.all_gather(spread, "y", axis=0, tiled=True)
    key_block, value_block = jnp.split(everything, (HEAD,), axis=1)

    turned = turned[:, :heads_half].astype(jnp.bfloat16).reshape(2, tok_dev, half_query)
    mine = jnp.where(side == 0, turned[0], turned[1])
    swapped = lax.ppermute(jnp.where(side == 0, turned[1], turned[0]), "pair", swap)
    query = jnp.concatenate(
        (jnp.where(side == 0, mine, swapped), jnp.where(side == 0, swapped, mine)), axis=1
    ).reshape(tok_dev, group_size, HEAD)

    length = key_block.shape[0]
    scores = jnp.einsum(
        "tgd,sd->gts", query, key_block, preferred_element_type=jnp.float32
    ) * (1.0 / math.sqrt(HEAD))
    query_positions = tok_index * tok_dev + jnp.arange(tok_dev, dtype=jnp.int32)
    key_positions = jnp.arange(length, dtype=jnp.int32)
    allowed = (doc_ids[:, None] == doc_block[None, :]) & (
        key_positions[None, :] <= query_positions[:, None]
    )
    scores = jnp.where(allowed, scores, -1e30)
    highest = jnp.max(scores, axis=2, keepdims=True)
    weights = jnp.where(allowed, jnp.exp(scores - highest), 0.0)
    totals = jnp.sum(weights, axis=2)
    accumulated = jnp.einsum(
        "gts,sd->gtd",
        weights.astype(jnp.bfloat16),
        value_block,
        preferred_element_type=jnp.float32,
    )
    attended = (
        (accumulated / totals[..., None])
        .transpose(1, 0, 2)
        .reshape(tok_dev, group_size * HEAD)
        .astype(jnp.bfloat16)
    )
    out_peak = to_everyone(jnp.max(jnp.abs(attended), axis=0), TOK)
    out_scale = jnp.max(out_peak, axis=0).astype(jnp.float32)
    return (
        attended,
        out_scale,
        folded_gain,
        codes[0],
        codes[1],
        codes[2],
        scales[0],
        scales[1],
        scales[2],
    )


def solution(mesh):
    split = Mesh(mesh.devices.reshape(8, 4, 2, 4, 2), ("y", "z", "pair", "x", "core"))
    placed = (P(TOK, None), P(), P(TOK, TP), P(TOK, TP), P(TOK, TP), P(TOK))
    return jax.shard_map(
        on_device,
        mesh=split,
        in_specs=placed,
        out_specs=(
            P(TOK, TP),
            P(TP),
            P(TOK_TP),
            P(TOK_TP, None),
            P(TOK_TP, None),
            P(TOK_TP, None),
            P(TP),
            P(TP),
            P(TP),
        ),
        check_vma=False,
    )
```

```python
import math

import jax
import jax.numpy as jnp
from jax import lax
from jax.sharding import Mesh
from jax.sharding import PartitionSpec as P

HEAD = 128
KVH = 8
QHEADS = 32
LINE = ("z", "pair")
TOK = ("y", "z", "pair")
TP = ("x", "core")
TOK_TP = TOK + TP


def exchange(parts, axis):
    return lax.all_to_all(parts, axis, split_axis=0, concat_axis=0, tiled=True)


def to_everyone(shard, axis):
    return exchange(jnp.broadcast_to(shard, (lax.axis_size(axis), *shard.shape)), axis)


def to_sides(even, odd):
    halves = jnp.stack((even, odd))
    sent = jnp.broadcast_to(halves, (lax.axis_size("z"), *halves.shape))
    return exchange(sent.reshape(-1, *even.shape), LINE).reshape(-1, even.shape[1])


def present(array):
    first = array.reshape(-1)[0]
    return first < 1e30


def in_pair_order(even, own, other):
    return jnp.concatenate(
        (jnp.where(even, own, other), jnp.where(even, other, own)), axis=0
    )


def rotate(states, positions):
    half = states.shape[-1] // 2
    inverse = jnp.exp(
        jnp.arange(half, dtype=jnp.float32) * (-2.0 * math.log(10000.0) / states.shape[-1])
    )
    angles = positions[:, None] * inverse[None, :]
    cosine = jnp.cos(angles)[:, None, :]
    sine = jnp.sin(angles)[:, None, :]
    first = states[..., :half]
    second = states[..., half:]
    return jnp.concatenate(
        [first * cosine - second * sine, second * cosine + first * sine], axis=-1
    )


def smooth_from(input_peak, weight_peak):
    return jnp.sqrt(jnp.maximum(input_peak, 1e-05)) / jnp.sqrt(jnp.maximum(weight_peak, 1e-05))


def on_device(hidden, norm_gain, w_query, w_key, w_value, doc_ids):
    tok_dev, width = hidden.shape
    row_count = w_query.shape[0]
    tok_count = lax.axis_size(TOK)
    tp_count = lax.axis_size(TP)
    tok_index = lax.axis_index(TOK)
    tp_index = lax.axis_index(TP)
    side = lax.axis_index("pair")
    core = lax.axis_index("core")
    line = lax.axis_size("z") * 2
    sub_rows = row_count // tp_count
    widths = (w_query.shape[1], w_key.shape[1], w_value.shape[1])
    cuts = (widths[0], widths[0] + widths[1])
    columns = sum(widths)
    half_query = widths[0] // 2
    group_size = QHEADS // KVH

    along_z = to_sides(w_key, w_value)
    gathered_last = lax.all_gather(along_z, "y", axis=0, tiled=True)

    states = hidden.astype(jnp.float32)
    inverse_rms = lax.rsqrt(jnp.mean(states * states, axis=1, keepdims=True) + 1e-05)
    normed = (states * inverse_rms * norm_gain[None, :]).astype(jnp.bfloat16)

    swap = [(0, 1), (1, 0)]
    channels = width // 2
    near = lax.ppermute(
        lax.dynamic_slice_in_dim(normed, core * channels, channels, axis=1), "pair", swap
    )
    held_query = jnp.where(present(normed), w_query, 0.0)
    along_z = to_sides(held_query[:, :half_query], held_query[:, half_query:])
    gathered_query = lax.all_gather(along_z, "y", axis=0, tiled=True)
    far = lax.ppermute(near, "core", swap)
    other = jnp.concatenate(
        (jnp.where(core == 0, near, far), jnp.where(core == 0, far, near)), axis=1
    )

    even = (side == 0) & present(along_z)
    both_rows = in_pair_order(even, normed, other)
    pair_positions = (tok_index - side) * tok_dev + jnp.arange(2 * tok_dev, dtype=jnp.int32)
    pair_positions = pair_positions.astype(jnp.float32)
    last = jnp.dot(both_rows, gathered_last, preferred_element_type=jnp.float32)
    turned = rotate(last[:, None, :], pair_positions)[:, 0]
    kept = jnp.where(side == 0, turned, last).astype(jnp.bfloat16)

    spread = to_everyone(kept, LINE).reshape(line // 2, 2, 2 * tok_dev, HEAD)
    sent_y = jnp.concatenate(
        (spread[:, 0].reshape(-1, HEAD), spread[:, 1].reshape(-1, HEAD)), axis=1
    )
    everything = lax.all_gather(sent_y, "y", axis=0, tiled=True)
    key_block, value_block = jnp.split(everything, (HEAD,), axis=1)

    peaks = jnp.max(jnp.abs(normed), axis=0).reshape(tok_count, row_count)
    peaks = jnp.where(present(spread), peaks, 0.0)
    docs = jnp.broadcast_to(doc_ids.astype(jnp.bfloat16), (tok_count, tok_dev))
    arrived = exchange(jnp.concatenate((peaks, docs), axis=1), TOK)
    input_peak = jnp.max(arrived[:, :row_count], axis=0).astype(jnp.float32)
    doc_block = arrived[:, row_count:].astype(jnp.int32).reshape(tok_count * tok_dev)

    block = jnp.concatenate((w_query, w_key, w_value), axis=1)
    row_peak = jnp.max(jnp.abs(block), axis=1)
    sent = jnp.concatenate(
        (
            block.reshape(tp_count, sub_rows * columns),
            jnp.broadcast_to(row_peak, (tp_count, row_count)),
        ),
        axis=1,
    )
    rows = exchange(sent, TP)
    weight_peak = jnp.max(rows[:, sub_rows * columns :], axis=0).astype(jnp.float32)
    own_rows = rows[:, : sub_rows * columns].reshape(tp_count, sub_rows, columns)

    smoothing = smooth_from(input_peak, weight_peak)
    column_peak = jnp.max(jnp.abs(smoothing[:, None] * block.astype(jnp.float32)), axis=0)
    column_peak = jnp.max(to_everyone(column_peak, TOK), axis=0)
    scale = jnp.maximum(column_peak, 1e-05) / 127.0
    all_scales = to_everyone(scale, TP)
    scales = jnp.split(scale, cuts)

    smooth_part = lax.dynamic_slice_in_dim(smoothing, tp_index * sub_rows, sub_rows)
    gain_part = lax.dynamic_slice_in_dim(
        norm_gain, tok_index * row_count + tp_index * sub_rows, sub_rows
    )
    folded_gain = gain_part / smooth_part
    coded = (
        smooth_part[None, :, None] * own_rows.astype(jnp.float32) / all_scales[:, None, :]
    )
    codes = tuple(
        part.transpose(1, 0, 2).reshape(sub_rows, tp_count * part.shape[2])
        for part in jnp.split(coded, cuts, axis=2)
    )

    even = (side == 0) & present(all_scales)
    both_rows = in_pair_order(even, normed, other)
    turned = jnp.dot(both_rows, gathered_query, preferred_element_type=jnp.float32)
    turned = rotate(turned.reshape(2 * tok_dev, -1, HEAD), pair_positions)
    turned = turned.astype(jnp.bfloat16).reshape(2, tok_dev, half_query)
    mine = jnp.where(side == 0, turned[0], turned[1])
    swapped = lax.ppermute(jnp.where(side == 0, turned[1], turned[0]), "pair", swap)
    query = jnp.concatenate(
        (jnp.where(side == 0, mine, swapped), jnp.where(side == 0, swapped, mine)), axis=1
    ).reshape(tok_dev, 1, group_size, HEAD)

    length = key_block.shape[0]
    scores = jnp.einsum(
        "tkgd,skd->kgts", query, key_block[:, None, :], preferred_element_type=jnp.float32
    ) * (1.0 / math.sqrt(HEAD))
    query_positions = tok_index * tok_dev + jnp.arange(tok_dev, dtype=jnp.int32)
    key_positions = jnp.arange(length, dtype=jnp.int32)
    allowed = (doc_ids[:, None] == doc_block[None, :]) & (
        key_positions[None, :] <= query_positions[:, None]
    )
    scores = jnp.where(allowed, scores, -1e30)
    highest = jnp.max(scores, axis=3, keepdims=True)
    weights = jnp.where(allowed, jnp.exp(scores - highest), 0.0)
    totals = jnp.sum(weights, axis=3)
    accumulated = jnp.einsum(
        "kgts,skd->kgtd",
        weights.astype(jnp.bfloat16),
        value_block[:, None, :],
        preferred_element_type=jnp.float32,
    )
    attended = (
        (accumulated / totals[..., None])
        .transpose(2, 0, 1, 3)
        .reshape(tok_dev, group_size * HEAD)
        .astype(jnp.bfloat16)
    )
    out_peak = jnp.max(jnp.abs(attended), axis=0)
    out_peak = jnp.max(to_everyone(out_peak, LINE), axis=0)
    out_scale = jnp.max(to_everyone(out_peak, "y"), axis=0).astype(jnp.float32)
    return (
        attended,
        out_scale,
        folded_gain,
        codes[0],
        codes[1],
        codes[2],
        scales[0],
        scales[1],
        scales[2],
    )


def solution(mesh):
    split = Mesh(mesh.devices.reshape(8, 4, 2, 4, 2), ("y", "z", "pair", "x", "core"))
    placed = (P(TOK, None), P(), P(TOK, TP), P(TOK, TP), P(TOK, TP), P(TOK))
    return jax.shard_map(
        on_device,
        mesh=split,
        in_specs=placed,
        out_specs=(
            P(TOK, TP),
            P(TP),
            P(TOK_TP),
            P(TOK_TP, None),
            P(TOK_TP, None),
            P(TOK_TP, None),
            P(TP),
            P(TP),
            P(TP),
        ),
        check_vma=False,
    )
```

```python
import math

import jax
import jax.numpy as jnp
from jax import lax
from jax.sharding import Mesh
from jax.sharding import PartitionSpec as P

HEAD = 128
KVH = 8
QHEADS = 32
LINE = ("z", "pair")
TOK = ("y", "z", "pair")
TP = ("x", "core")
TOK_TP = TOK + TP


def exchange(parts, axis):
    return lax.all_to_all(parts, axis, split_axis=0, concat_axis=0, tiled=True)


def to_everyone(shard, axis):
    return exchange(jnp.broadcast_to(shard, (lax.axis_size(axis), *shard.shape)), axis)


def to_sides(even, odd):
    halves = jnp.stack((even, odd))
    sent = jnp.broadcast_to(halves, (lax.axis_size("z"), *halves.shape))
    return exchange(sent.reshape(-1, *even.shape), LINE).reshape(-1, even.shape[1])


def present(array):
    first = array.reshape(-1)[0]
    return first < 1e30


def in_pair_order(even, own, other):
    return jnp.concatenate(
        (jnp.where(even, own, other), jnp.where(even, other, own)), axis=0
    )


def rotate(states, positions):
    half = states.shape[-1] // 2
    inverse = jnp.exp(
        jnp.arange(half, dtype=jnp.float32) * (-2.0 * math.log(10000.0) / states.shape[-1])
    )
    angles = positions[:, None] * inverse[None, :]
    cosine = jnp.cos(angles)[:, None, :]
    sine = jnp.sin(angles)[:, None, :]
    first = states[..., :half]
    second = states[..., half:]
    return jnp.concatenate(
        [first * cosine - second * sine, second * cosine + first * sine], axis=-1
    )


def smooth_from(input_peak, weight_peak):
    return jnp.sqrt(jnp.maximum(input_peak, 1e-05)) / jnp.sqrt(jnp.maximum(weight_peak, 1e-05))


def on_device(hidden, norm_gain, w_query, w_key, w_value, doc_ids):
    tok_dev, width = hidden.shape
    row_count = w_query.shape[0]
    tok_count = lax.axis_size(TOK)
    tp_count = lax.axis_size(TP)
    tok_index = lax.axis_index(TOK)
    tp_index = lax.axis_index(TP)
    side = lax.axis_index("pair")
    core = lax.axis_index("core")
    line = lax.axis_size("z") * 2
    sub_rows = row_count // tp_count
    widths = (w_query.shape[1], w_key.shape[1], w_value.shape[1])
    cuts = (widths[0], widths[0] + widths[1])
    columns = sum(widths)
    half_query = widths[0] // 2
    group_size = QHEADS // KVH

    along_z = to_sides(w_key, w_value)
    gathered_last = lax.all_gather(along_z, "y", axis=0, tiled=True)

    states = hidden.astype(jnp.float32)
    inverse_rms = lax.rsqrt(jnp.mean(states * states, axis=1, keepdims=True) + 1e-05)
    normed = (states * inverse_rms * norm_gain[None, :]).astype(jnp.bfloat16)

    swap = [(0, 1), (1, 0)]
    channels = width // 2
    near = lax.ppermute(
        lax.dynamic_slice_in_dim(normed, core * channels, channels, axis=1), "pair", swap
    )
    held_query = jnp.where(present(normed), w_query, 0.0)
    along_z = to_sides(held_query[:, :half_query], held_query[:, half_query:])
    gathered_query = lax.all_gather(along_z, "y", axis=0, tiled=True)
    far = lax.ppermute(near, "core", swap)
    other = jnp.concatenate(
        (jnp.where(core == 0, near, far), jnp.where(core == 0, far, near)), axis=1
    )

    even = (side == 0) & present(along_z)
    both_rows = in_pair_order(even, normed, other)
    pair_positions = (tok_index - side) * tok_dev + jnp.arange(2 * tok_dev, dtype=jnp.int32)
    pair_positions = pair_positions.astype(jnp.float32)
    last = jnp.dot(both_rows, gathered_last, preferred_element_type=jnp.float32)
    turned = rotate(last[:, None, :], pair_positions)[:, 0]
    kept = jnp.where(side == 0, turned, last).astype(jnp.bfloat16)

    spread = to_everyone(kept, LINE).reshape(line // 2, 2, 2 * tok_dev, HEAD)
    sent_y = jnp.concatenate(
        (spread[:, 0].reshape(-1, HEAD), spread[:, 1].reshape(-1, HEAD)), axis=1
    )
    everything = lax.all_gather(sent_y, "y", axis=0, tiled=True)
    key_block, value_block = jnp.split(everything, (HEAD,), axis=1)

    peaks = jnp.max(jnp.abs(normed), axis=0).reshape(tok_count, row_count)
    peaks = jnp.where(present(along_z), peaks, 0.0)
    docs = jnp.broadcast_to(doc_ids.astype(jnp.bfloat16), (tok_count, tok_dev))
    arrived = exchange(jnp.concatenate((peaks, docs), axis=1), TOK)
    input_peak = jnp.max(arrived[:, :row_count], axis=0).astype(jnp.float32)
    doc_block = arrived[:, row_count:].astype(jnp.int32).reshape(tok_count * tok_dev)

    block = jnp.concatenate((w_query, w_key, w_value), axis=1)
    row_peak = jnp.max(jnp.abs(block), axis=1)
    sent = jnp.concatenate(
        (
            block.reshape(tp_count, sub_rows * columns),
            jnp.broadcast_to(row_peak, (tp_count, row_count)),
        ),
        axis=1,
    )
    rows = exchange(sent, TP)
    weight_peak = jnp.max(rows[:, sub_rows * columns :], axis=0).astype(jnp.float32)
    own_rows = rows[:, : sub_rows * columns].reshape(tp_count, sub_rows, columns)

    smoothing = smooth_from(input_peak, weight_peak)
    column_peak = jnp.max(jnp.abs(smoothing[:, None] * block.astype(jnp.float32)), axis=0)
    column_peak = jnp.where(present(spread), column_peak, 0.0)
    column_peak = jnp.max(to_everyone(column_peak, LINE), axis=0)
    column_peak = jnp.max(to_everyone(column_peak, "y"), axis=0)
    scale = jnp.maximum(column_peak, 1e-05) / 127.0
    all_scales = to_everyone(scale, TP)
    scales = jnp.split(scale, cuts)

    smooth_part = lax.dynamic_slice_in_dim(smoothing, tp_index * sub_rows, sub_rows)
    gain_part = lax.dynamic_slice_in_dim(
        norm_gain, tok_index * row_count + tp_index * sub_rows, sub_rows
    )
    folded_gain = gain_part / smooth_part
    coded = (
        smooth_part[None, :, None] * own_rows.astype(jnp.float32) / all_scales[:, None, :]
    )
    codes = tuple(
        part.transpose(1, 0, 2).reshape(sub_rows, tp_count * part.shape[2])
        for part in jnp.split(coded, cuts, axis=2)
    )

    even = (side == 0) & present(all_scales)
    both_rows = in_pair_order(even, normed, other)
    turned = jnp.dot(both_rows, gathered_query, preferred_element_type=jnp.float32)
    turned = rotate(turned.reshape(2 * tok_dev, -1, HEAD), pair_positions)
    turned = turned.astype(jnp.bfloat16).reshape(2, tok_dev, half_query)
    mine = jnp.where(side == 0, turned[0], turned[1])
    swapped = lax.ppermute(jnp.where(side == 0, turned[1], turned[0]), "pair", swap)
    query = jnp.concatenate(
        (jnp.where(side == 0, mine, swapped), jnp.where(side == 0, swapped, mine)), axis=1
    ).reshape(tok_dev, 1, group_size, HEAD)

    length = key_block.shape[0]
    scores = jnp.einsum(
        "tkgd,skd->kgts", query, key_block[:, None, :], preferred_element_type=jnp.float32
    ) * (1.0 / math.sqrt(HEAD))
    query_positions = tok_index * tok_dev + jnp.arange(tok_dev, dtype=jnp.int32)
    key_positions = jnp.arange(length, dtype=jnp.int32)
    allowed = (doc_ids[:, None] == doc_block[None, :]) & (
        key_positions[None, :] <= query_positions[:, None]
    )
    scores = jnp.where(allowed, scores, -1e30)
    highest = jnp.max(scores, axis=3, keepdims=True)
    weights = jnp.where(allowed, jnp.exp(scores - highest), 0.0)
    totals = jnp.sum(weights, axis=3)
    accumulated = jnp.einsum(
        "kgts,skd->kgtd",
        weights.astype(jnp.bfloat16),
        value_block[:, None, :],
        preferred_element_type=jnp.float32,
    )
    attended = (
        (accumulated / totals[..., None])
        .transpose(2, 0, 1, 3)
        .reshape(tok_dev, group_size * HEAD)
        .astype(jnp.bfloat16)
    )
    out_peak = jnp.max(jnp.abs(attended), axis=0).astype(jnp.float32)
    out_peak = jnp.max(to_everyone(out_peak, LINE), axis=0)
    out_scale = jnp.max(to_everyone(out_peak, "y"), axis=0)
    return (
        attended,
        out_scale,
        folded_gain,
        codes[0],
        codes[1],
        codes[2],
        scales[0],
        scales[1],
        scales[2],
    )


def solution(mesh):
    split = Mesh(mesh.devices.reshape(8, 4, 2, 4, 2), ("y", "z", "pair", "x", "core"))
    placed = (P(TOK, None), P(), P(TOK, TP), P(TOK, TP), P(TOK, TP), P(TOK))
    return jax.shard_map(
        on_device,
        mesh=split,
        in_specs=placed,
        out_specs=(
            P(TOK, TP),
            P(TP),
            P(TOK_TP),
            P(TOK_TP, None),
            P(TOK_TP, None),
            P(TOK_TP, None),
            P(TP),
            P(TP),
            P(TP),
        ),
        check_vma=False,
    )
```

```python
import math

import jax
import jax.numpy as jnp
from jax import lax
from jax.sharding import Mesh
from jax.sharding import PartitionSpec as P

HEAD = 128
KVH = 8
QHEADS = 32
LINE = ("z", "pair")
TOK = ("y", "z", "pair")
TP = ("x", "core")
TOK_TP = TOK + TP


def exchange(parts, axis):
    return lax.all_to_all(parts, axis, split_axis=0, concat_axis=0, tiled=True)


def to_everyone(shard, axis):
    return exchange(jnp.broadcast_to(shard, (lax.axis_size(axis), *shard.shape)), axis)


def to_sides(even, odd):
    halves = jnp.stack((even, odd))
    sent = jnp.broadcast_to(halves, (lax.axis_size("z"), *halves.shape))
    return exchange(sent.reshape(-1, *even.shape), LINE).reshape(-1, even.shape[1])


def present(array):
    first = array.reshape(-1)[0]
    return first < 1e30


def in_pair_order(even, own, other):
    return jnp.concatenate(
        (jnp.where(even, own, other), jnp.where(even, other, own)), axis=0
    )


def rotate(states, positions):
    half = states.shape[-1] // 2
    inverse = jnp.exp(
        jnp.arange(half, dtype=jnp.float32) * (-2.0 * math.log(10000.0) / states.shape[-1])
    )
    angles = positions[:, None] * inverse[None, :]
    cosine = jnp.cos(angles)[:, None, :]
    sine = jnp.sin(angles)[:, None, :]
    first = states[..., :half]
    second = states[..., half:]
    return jnp.concatenate(
        [first * cosine - second * sine, second * cosine + first * sine], axis=-1
    )


def smooth_from(input_peak, weight_peak):
    return jnp.sqrt(jnp.maximum(input_peak, 1e-05)) / jnp.sqrt(jnp.maximum(weight_peak, 1e-05))


def on_device(hidden, norm_gain, w_query, w_key, w_value, doc_ids):
    tok_dev, width = hidden.shape
    row_count = w_query.shape[0]
    tok_count = lax.axis_size(TOK)
    tp_count = lax.axis_size(TP)
    tok_index = lax.axis_index(TOK)
    tp_index = lax.axis_index(TP)
    side = lax.axis_index("pair")
    core = lax.axis_index("core")
    line = lax.axis_size(LINE)
    tall = lax.axis_size("y")
    sub_rows = row_count // tp_count
    widths = (w_query.shape[1], w_key.shape[1], w_value.shape[1])
    cuts = (widths[0], widths[0] + widths[1])
    columns = sum(widths)
    half_query = widths[0] // 2
    group_size = QHEADS // KVH

    along_z = to_sides(w_key, w_value)
    gathered_last = lax.all_gather(along_z, "y", axis=0, tiled=True)

    states = hidden.astype(jnp.float32)
    inverse_rms = lax.rsqrt(jnp.mean(states * states, axis=1, keepdims=True) + 1e-05)
    normed = (states * inverse_rms * norm_gain[None, :]).astype(jnp.bfloat16)

    swap = [(0, 1), (1, 0)]
    channels = width // 2
    near = lax.ppermute(
        lax.dynamic_slice_in_dim(normed, core * channels, channels, axis=1), "pair", swap
    )
    heads_wide = half_query
    peaks = jnp.max(jnp.abs(normed), axis=0).reshape(tall, line, row_count)
    peaks = peaks.transpose(1, 0, 2).reshape(line, -1, heads_wide)
    docs = jnp.pad(doc_ids.astype(jnp.bfloat16), (0, heads_wide - tok_dev))
    docs = jnp.broadcast_to(docs, (line, 1, heads_wide))
    peak_rows = peaks.shape[1]
    blank = jnp.zeros((line, 15 - peak_rows, heads_wide), jnp.bfloat16)
    halves = jnp.stack((w_query[:, :half_query], w_query[:, half_query:]))
    sent = jnp.broadcast_to(halves, (line // 2, *halves.shape))
    sent = sent.reshape(line, row_count, heads_wide)
    along_z = exchange(jnp.concatenate((sent, peaks, docs, blank), axis=1), LINE)
    gathered_query = lax.all_gather(
        along_z[:, :row_count].reshape(-1, heads_wide), "y", axis=0, tiled=True
    )
    riders = along_z[:, row_count:]
    peaks = jnp.max(riders[:, :peak_rows], axis=0).reshape(tall, row_count)
    docs = riders[:, peak_rows, :tok_dev].reshape(line * tok_dev)
    docs = jnp.broadcast_to(docs, (tall, line * tok_dev))
    arrived = exchange(jnp.concatenate((peaks, docs), axis=1), "y")
    input_peak = jnp.max(arrived[:, :row_count], axis=0).astype(jnp.float32)
    doc_block = arrived[:, row_count:].astype(jnp.int32).reshape(tok_count * tok_dev)
    far = lax.ppermute(near, "core", swap)
    other = jnp.concatenate(
        (jnp.where(core == 0, near, far), jnp.where(core == 0, far, near)), axis=1
    )

    even = (side == 0) & present(along_z)
    both_rows = in_pair_order(even, normed, other)
    pair_positions = (tok_index - side) * tok_dev + jnp.arange(2 * tok_dev, dtype=jnp.int32)
    pair_positions = pair_positions.astype(jnp.float32)
    last = jnp.dot(both_rows, gathered_last, preferred_element_type=jnp.float32)
    turned = rotate(last[:, None, :], pair_positions)[:, 0]
    kept = jnp.where(side == 0, turned, last).astype(jnp.bfloat16)

    spread = to_everyone(kept, LINE).reshape(line // 2, 2, 2 * tok_dev, HEAD)
    sent_y = jnp.concatenate(
        (spread[:, 0].reshape(-1, HEAD), spread[:, 1].reshape(-1, HEAD)), axis=1
    )
    everything = lax.all_gather(sent_y, "y", axis=0, tiled=True)
    key_block, value_block = jnp.split(everything, (HEAD,), axis=1)

    block = jnp.concatenate((w_query, w_key, w_value), axis=1)
    row_peak = jnp.max(jnp.abs(block), axis=1)
    sent = jnp.concatenate(
        (
            block.reshape(tp_count, sub_rows * columns),
            jnp.broadcast_to(row_peak, (tp_count, row_count)),
        ),
        axis=1,
    )
    rows = exchange(sent, TP)
    weight_peak = jnp.max(rows[:, sub_rows * columns :], axis=0).astype(jnp.float32)
    own_rows = rows[:, : sub_rows * columns].reshape(tp_count, sub_rows, columns)

    smoothing = smooth_from(input_peak, weight_peak)
    column_peak = jnp.max(jnp.abs(smoothing[:, None] * block.astype(jnp.float32)), axis=0)
    column_peak = jnp.where(present(spread), column_peak, 0.0)
    column_peak = jnp.max(to_everyone(column_peak, LINE), axis=0)
    column_peak = jnp.max(to_everyone(column_peak, "y"), axis=0)
    scale = jnp.maximum(column_peak, 1e-05) / 127.0
    all_scales = to_everyone(scale, TP)
    scales = jnp.split(scale, cuts)

    smooth_part = lax.dynamic_slice_in_dim(smoothing, tp_index * sub_rows, sub_rows)
    gain_part = lax.dynamic_slice_in_dim(
        norm_gain, tok_index * row_count + tp_index * sub_rows, sub_rows
    )
    folded_gain = gain_part / smooth_part
    coded = (
        smooth_part[None, :, None] * own_rows.astype(jnp.float32) / all_scales[:, None, :]
    )
    codes = tuple(
        part.transpose(1, 0, 2).reshape(sub_rows, tp_count * part.shape[2])
        for part in jnp.split(coded, cuts, axis=2)
    )

    even = (side == 0) & present(all_scales)
    both_rows = in_pair_order(even, normed, other)
    turned = jnp.dot(both_rows, gathered_query, preferred_element_type=jnp.float32)
    turned = rotate(turned.reshape(2 * tok_dev, -1, HEAD), pair_positions)
    turned = turned.astype(jnp.bfloat16).reshape(2, tok_dev, half_query)
    mine = jnp.where(side == 0, turned[0], turned[1])
    swapped = lax.ppermute(jnp.where(side == 0, turned[1], turned[0]), "pair", swap)
    query = jnp.concatenate(
        (jnp.where(side == 0, mine, swapped), jnp.where(side == 0, swapped, mine)), axis=1
    ).reshape(tok_dev, 1, group_size, HEAD)

    length = key_block.shape[0]
    scores = jnp.einsum(
        "tkgd,skd->kgts", query, key_block[:, None, :], preferred_element_type=jnp.float32
    ) * (1.0 / math.sqrt(HEAD))
    query_positions = tok_index * tok_dev + jnp.arange(tok_dev, dtype=jnp.int32)
    key_positions = jnp.arange(length, dtype=jnp.int32)
    allowed = (doc_ids[:, None] == doc_block[None, :]) & (
        key_positions[None, :] <= query_positions[:, None]
    )
    scores = jnp.where(allowed, scores, -1e30)
    highest = jnp.max(scores, axis=3, keepdims=True)
    weights = jnp.where(allowed, jnp.exp(scores - highest), 0.0)
    totals = jnp.sum(weights, axis=3)
    accumulated = jnp.einsum(
        "kgts,skd->kgtd",
        weights.astype(jnp.bfloat16),
        value_block[:, None, :],
        preferred_element_type=jnp.float32,
    )
    attended = (
        (accumulated / totals[..., None])
        .transpose(2, 0, 1, 3)
        .reshape(tok_dev, group_size * HEAD)
        .astype(jnp.bfloat16)
    )
    out_peak = jnp.max(jnp.abs(attended), axis=0).astype(jnp.float32)
    out_scale = jnp.max(to_everyone(out_peak, TOK), axis=0)
    return (
        attended,
        out_scale,
        folded_gain,
        codes[0],
        codes[1],
        codes[2],
        scales[0],
        scales[1],
        scales[2],
    )


def solution(mesh):
    split = Mesh(mesh.devices.reshape(8, 4, 2, 4, 2), ("y", "z", "pair", "x", "core"))
    placed = (P(TOK, None), P(), P(TOK, TP), P(TOK, TP), P(TOK, TP), P(TOK))
    return jax.shard_map(
        on_device,
        mesh=split,
        in_specs=placed,
        out_specs=(
            P(TOK, TP),
            P(TP),
            P(TOK_TP),
            P(TOK_TP, None),
            P(TOK_TP, None),
            P(TOK_TP, None),
            P(TP),
            P(TP),
            P(TP),
        ),
        check_vma=False,
    )
```

```python
import math

import jax
import jax.numpy as jnp
from jax import lax
from jax.experimental import pallas as pl
from jax.experimental.pallas import tpu as pltpu
from jax.sharding import Mesh
from jax.sharding import PartitionSpec as P

HEAD = 128
KVH = 8
QHEADS = 32
LINE = ("z", "pair")
TOK = ("y", "z", "pair")
TP = ("x", "core")
TOK_TP = TOK + TP


def exchange(parts, axis):
    return lax.all_to_all(parts, axis, split_axis=0, concat_axis=0, tiled=True)


def to_everyone(shard, axis):
    return exchange(jnp.broadcast_to(shard, (lax.axis_size(axis), *shard.shape)), axis)


def to_sides(even, odd):
    halves = jnp.stack((even, odd))
    sent = jnp.broadcast_to(halves, (lax.axis_size("z"), *halves.shape))
    return exchange(sent.reshape(-1, *even.shape), LINE).reshape(-1, even.shape[1])


def present(array):
    first = array.reshape(-1)[0]
    return first < 1e30


def in_pair_order(even, own, other):
    return jnp.concatenate(
        (jnp.where(even, own, other), jnp.where(even, other, own)), axis=0
    )


def rotate(states, positions):
    half = states.shape[-1] // 2
    inverse = jnp.exp(
        jnp.arange(half, dtype=jnp.float32) * (-2.0 * math.log(10000.0) / states.shape[-1])
    )
    angles = positions[:, None] * inverse[None, :]
    cosine = jnp.cos(angles)[:, None, :]
    sine = jnp.sin(angles)[:, None, :]
    first = states[..., :half]
    second = states[..., half:]
    return jnp.concatenate(
        [first * cosine - second * sine, second * cosine + first * sine], axis=-1
    )


def attend(span, bounds, query, keyed, tok_dev):
    total, head = query.shape
    length = keyed.shape[0]
    block = 512
    group = total // tok_dev
    factor = 1.0 / math.sqrt(head)

    def kernel(span_ref, bounds_ref, query_ref, keyed_ref, out_ref, peak_ref, score_ref):
        first, last = span_ref[0], span_ref[1]
        start_most, token_least = span_ref[2], span_ref[3]
        queries = query_ref[...]

        def scored(index, highest):
            base = index * block
            keys = keyed_ref[pl.ds(base, block), :head]
            score_ref[index] = lax.dot_general(
                queries, keys, (((1,), (1,)), ((), ())), preferred_element_type=jnp.float32
            )

            @pl.when((base < start_most) | (base + block - 1 > token_least))
            def _():
                place = base + lax.broadcasted_iota(jnp.int32, (total, block), 1)
                inside = (place >= bounds_ref[:, :1]) & (place <= bounds_ref[:, 1:])
                score_ref[index] = jnp.where(inside, score_ref[index], -1e30)

            scores = score_ref[index]
            for k in range(0, block, 128):
                highest = jnp.maximum(highest, scores[:, k : k + 128])
            return highest

        highest = lax.fori_loop(
            first, last, scored, jnp.full((total, 128), -1e30, jnp.float32)
        )
        highest = jnp.max(highest, axis=1, keepdims=True)

        def weighted(index, carried):
            sums, gathered = carried
            weights = jnp.exp((score_ref[index] - highest) * factor)
            for k in range(0, block, 128):
                sums = sums + weights[:, k : k + 128]
            values = keyed_ref[pl.ds(index * block, block), head:]
            gathered = gathered + jnp.dot(
                weights.astype(jnp.bfloat16), values, preferred_element_type=jnp.float32
            )
            return sums, gathered

        zeros = jnp.zeros((total, 128), jnp.float32)
        sums, gathered = lax.fori_loop(first, last, weighted, (zeros, zeros))
        attended = (gathered / jnp.sum(sums, axis=1, keepdims=True)).astype(jnp.bfloat16)
        for g in range(group):
            part = attended[g * tok_dev : (g + 1) * tok_dev]
            out_ref[:, g * head : (g + 1) * head] = part
            peak_ref[:, g * head : (g + 1) * head] = jnp.max(
                jnp.abs(part.astype(jnp.float32)), axis=0, keepdims=True
            )

    in_vmem = pl.BlockSpec(memory_space=pltpu.VMEM)
    return pl.pallas_call(
        kernel,
        out_shape=(
            jax.ShapeDtypeStruct((tok_dev, group * head), jnp.bfloat16),
            jax.ShapeDtypeStruct((1, group * head), jnp.float32),
        ),
        in_specs=[pl.BlockSpec(memory_space=pltpu.SMEM), in_vmem, in_vmem, in_vmem],
        out_specs=(in_vmem, in_vmem),
        scratch_shapes=[pltpu.VMEM((length // block, total, block), jnp.float32)],
        name="attend",
        compiler_params=pltpu.CompilerParams(vmem_limit_bytes=32 * 1024 * 1024),
    )(span, bounds, query, keyed)


def smooth_from(input_peak, weight_peak):
    return jnp.sqrt(jnp.maximum(input_peak, 1e-05)) / jnp.sqrt(jnp.maximum(weight_peak, 1e-05))


def on_device(hidden, norm_gain, w_query, w_key, w_value, doc_ids):
    tok_dev, width = hidden.shape
    row_count = w_query.shape[0]
    tok_count = lax.axis_size(TOK)
    tp_count = lax.axis_size(TP)
    tok_index = lax.axis_index(TOK)
    tp_index = lax.axis_index(TP)
    side = lax.axis_index("pair")
    core = lax.axis_index("core")
    line = lax.axis_size(LINE)
    tall = lax.axis_size("y")
    sub_rows = row_count // tp_count
    widths = (w_query.shape[1], w_key.shape[1], w_value.shape[1])
    cuts = (widths[0], widths[0] + widths[1])
    columns = sum(widths)
    half_query = widths[0] // 2
    group_size = QHEADS // KVH

    along_z = to_sides(w_key, w_value)
    gathered_last = lax.all_gather(along_z, "y", axis=0, tiled=True)

    states = hidden.astype(jnp.float32)
    inverse_rms = lax.rsqrt(jnp.mean(states * states, axis=1, keepdims=True) + 1e-05)
    normed = (states * inverse_rms * norm_gain[None, :]).astype(jnp.bfloat16)

    swap = [(0, 1), (1, 0)]
    channels = width // 2
    near = lax.ppermute(
        lax.dynamic_slice_in_dim(normed, core * channels, channels, axis=1), "pair", swap
    )
    heads_wide = half_query
    peaks = jnp.max(jnp.abs(normed), axis=0).reshape(tall, line, row_count)
    peaks = peaks.transpose(1, 0, 2).reshape(line, -1, heads_wide)
    docs = jnp.pad(doc_ids.astype(jnp.bfloat16), (0, heads_wide - tok_dev))
    docs = jnp.broadcast_to(docs, (line, 1, heads_wide))
    peak_rows = peaks.shape[1]
    blank = jnp.zeros((line, 15 - peak_rows, heads_wide), jnp.bfloat16)
    halves = jnp.stack((w_query[:, :half_query], w_query[:, half_query:]))
    sent = jnp.broadcast_to(halves, (line // 2, *halves.shape))
    sent = sent.reshape(line, row_count, heads_wide)
    along_z = exchange(jnp.concatenate((sent, peaks, docs, blank), axis=1), LINE)
    gathered_query = lax.all_gather(
        along_z[:, :row_count].reshape(-1, heads_wide), "y", axis=0, tiled=True
    )
    riders = along_z[:, row_count:]
    peaks = jnp.max(riders[:, :peak_rows], axis=0).reshape(tall, row_count)
    docs = riders[:, peak_rows, :tok_dev].reshape(line * tok_dev)
    docs = jnp.broadcast_to(docs, (tall, line * tok_dev))
    arrived = exchange(jnp.concatenate((peaks, docs), axis=1), "y")
    input_peak = jnp.max(arrived[:, :row_count], axis=0).astype(jnp.float32)
    doc_block = arrived[:, row_count:].astype(jnp.int32).reshape(tok_count * tok_dev)
    far = lax.ppermute(near, "core", swap)
    other = jnp.concatenate(
        (jnp.where(core == 0, near, far), jnp.where(core == 0, far, near)), axis=1
    )

    even = (side == 0) & present(along_z)
    both_rows = in_pair_order(even, normed, other)
    pair_positions = (tok_index - side) * tok_dev + jnp.arange(2 * tok_dev, dtype=jnp.int32)
    pair_positions = pair_positions.astype(jnp.float32)
    last = jnp.dot(both_rows, gathered_last, preferred_element_type=jnp.float32)
    turned = rotate(last[:, None, :], pair_positions)[:, 0]
    kept = jnp.where(side == 0, turned, last).astype(jnp.bfloat16)

    spread = to_everyone(kept, LINE).reshape(line // 2, 2, 2 * tok_dev, HEAD)
    sent_y = jnp.concatenate(
        (spread[:, 0].reshape(-1, HEAD), spread[:, 1].reshape(-1, HEAD)), axis=1
    )
    everything = lax.all_gather(sent_y, "y", axis=0, tiled=True)

    block = jnp.concatenate((w_query, w_key, w_value), axis=1)
    row_peak = jnp.max(jnp.abs(block), axis=1)
    sent = jnp.concatenate(
        (
            block.reshape(tp_count, sub_rows * columns),
            jnp.broadcast_to(row_peak, (tp_count, row_count)),
        ),
        axis=1,
    )
    rows = exchange(sent, TP)
    weight_peak = jnp.max(rows[:, sub_rows * columns :], axis=0).astype(jnp.float32)
    own_rows = rows[:, : sub_rows * columns].reshape(tp_count, sub_rows, columns)

    smoothing = smooth_from(input_peak, weight_peak)
    column_peak = jnp.max(jnp.abs(smoothing[:, None] * block.astype(jnp.float32)), axis=0)
    column_peak = jnp.where(present(spread), column_peak, 0.0)
    column_peak = jnp.max(to_everyone(column_peak, LINE), axis=0)
    column_peak = jnp.max(to_everyone(column_peak, "y"), axis=0)
    scale = jnp.maximum(column_peak, 1e-05) / 127.0
    all_scales = to_everyone(scale, TP)
    scales = jnp.split(scale, cuts)

    smooth_part = lax.dynamic_slice_in_dim(smoothing, tp_index * sub_rows, sub_rows)
    gain_part = lax.dynamic_slice_in_dim(
        norm_gain, tok_index * row_count + tp_index * sub_rows, sub_rows
    )
    folded_gain = gain_part / smooth_part
    coded = (
        smooth_part[None, :, None] * own_rows.astype(jnp.float32) / all_scales[:, None, :]
    )
    codes = tuple(
        part.transpose(1, 0, 2).reshape(sub_rows, tp_count * part.shape[2])
        for part in jnp.split(coded, cuts, axis=2)
    )

    even = (side == 0) & present(all_scales)
    both_rows = in_pair_order(even, normed, other)
    turned = jnp.dot(both_rows, gathered_query, preferred_element_type=jnp.float32)
    turned = rotate(turned.reshape(2 * tok_dev, -1, HEAD), pair_positions)
    turned = turned.astype(jnp.bfloat16).reshape(2, tok_dev, half_query)
    mine = jnp.where(side == 0, turned[0], turned[1])
    swapped = lax.ppermute(jnp.where(side == 0, turned[1], turned[0]), "pair", swap)
    query = jnp.concatenate(
        (jnp.where(side == 0, mine, swapped), jnp.where(side == 0, swapped, mine)), axis=1
    ).reshape(tok_dev, group_size, HEAD)
    query = query.transpose(1, 0, 2).reshape(group_size * tok_dev, HEAD)

    places = tok_index * tok_dev + jnp.arange(tok_dev, dtype=jnp.int32)
    starts = jnp.sum((doc_block[None, :] < doc_ids[:, None]).astype(jnp.int32), axis=1)
    span = jnp.stack((starts[0] // 512, places[-1] // 512 + 1, starts[-1], places[0]))
    bounds = jnp.tile(jnp.stack((starts, places), axis=1), (group_size, 1))
    attended, out_peak = attend(span, bounds, query, everything, tok_dev)
    out_scale = jnp.max(to_everyone(out_peak[0], TOK), axis=0)
    return (
        attended,
        out_scale,
        folded_gain,
        codes[0],
        codes[1],
        codes[2],
        scales[0],
        scales[1],
        scales[2],
    )


def solution(mesh):
    split = Mesh(mesh.devices.reshape(8, 4, 2, 4, 2), ("y", "z", "pair", "x", "core"))
    placed = (P(TOK, None), P(), P(TOK, TP), P(TOK, TP), P(TOK, TP), P(TOK))
    return jax.shard_map(
        on_device,
        mesh=split,
        in_specs=placed,
        out_specs=(
            P(TOK, TP),
            P(TP),
            P(TOK_TP),
            P(TOK_TP, None),
            P(TOK_TP, None),
            P(TOK_TP, None),
            P(TP),
            P(TP),
            P(TP),
        ),
        check_vma=False,
    )
```

```python
import math

import jax
import jax.numpy as jnp
from jax import lax
from jax.sharding import Mesh
from jax.sharding import PartitionSpec as P

HEAD = 128
KVH = 8
QHEADS = 32
LINE = ("z", "pair")
TOK = ("y", "z", "pair")
TP = ("x", "core")
TOK_TP = TOK + TP


def exchange(parts, axis):
    return lax.all_to_all(parts, axis, split_axis=0, concat_axis=0, tiled=True)


def to_everyone(shard, axis):
    return exchange(jnp.broadcast_to(shard, (lax.axis_size(axis), *shard.shape)), axis)


def to_sides(even, odd):
    halves = jnp.stack((even, odd))
    sent = jnp.broadcast_to(halves, (lax.axis_size("z"), *halves.shape))
    return exchange(sent.reshape(-1, *even.shape), LINE).reshape(-1, even.shape[1])


def present(array):
    first = array.reshape(-1)[0]
    return first < 1e30


def in_pair_order(even, own, other):
    return jnp.concatenate(
        (jnp.where(even, own, other), jnp.where(even, other, own)), axis=0
    )


def rotate(states, positions):
    half = states.shape[-1] // 2
    inverse = jnp.exp(
        jnp.arange(half, dtype=jnp.float32) * (-2.0 * math.log(10000.0) / states.shape[-1])
    )
    angles = positions[:, None] * inverse[None, :]
    cosine = jnp.cos(angles)[:, None, :]
    sine = jnp.sin(angles)[:, None, :]
    first = states[..., :half]
    second = states[..., half:]
    return jnp.concatenate(
        [first * cosine - second * sine, second * cosine + first * sine], axis=-1
    )


def smooth_from(input_peak, weight_peak):
    return jnp.sqrt(jnp.maximum(input_peak, 1e-05)) / jnp.sqrt(jnp.maximum(weight_peak, 1e-05))


def on_device(hidden, norm_gain, w_query, w_key, w_value, doc_ids):
    tok_dev, width = hidden.shape
    row_count = w_query.shape[0]
    tok_count = lax.axis_size(TOK)
    tp_count = lax.axis_size(TP)
    tok_index = lax.axis_index(TOK)
    tp_index = lax.axis_index(TP)
    side = lax.axis_index("pair")
    core = lax.axis_index("core")
    line = lax.axis_size(LINE)
    tall = lax.axis_size("y")
    sub_rows = row_count // tp_count
    widths = (w_query.shape[1], w_key.shape[1], w_value.shape[1])
    cuts = (widths[0], widths[0] + widths[1])
    columns = sum(widths)
    half_query = widths[0] // 2
    group_size = QHEADS // KVH

    along_z = to_sides(w_key, w_value)
    gathered_last = lax.all_gather(along_z, "y", axis=0, tiled=True)

    states = hidden.astype(jnp.float32)
    inverse_rms = lax.rsqrt(jnp.mean(states * states, axis=1, keepdims=True) + 1e-05)
    normed = (states * inverse_rms * norm_gain[None, :]).astype(jnp.bfloat16)

    swap = [(0, 1), (1, 0)]
    channels = width // 2
    near = lax.ppermute(
        lax.dynamic_slice_in_dim(normed, core * channels, channels, axis=1), "pair", swap
    )
    heads_wide = half_query
    peaks = jnp.max(jnp.abs(normed), axis=0).reshape(tall, line, row_count)
    peaks = peaks.transpose(1, 0, 2).reshape(line, -1, heads_wide)
    docs = jnp.pad(doc_ids.astype(jnp.bfloat16), (0, heads_wide - tok_dev))
    docs = jnp.broadcast_to(docs, (line, 1, heads_wide))
    peak_rows = peaks.shape[1]
    blank = jnp.zeros((line, 15 - peak_rows, heads_wide), jnp.bfloat16)
    halves = jnp.stack((w_query[:, :half_query], w_query[:, half_query:]))
    sent = jnp.broadcast_to(halves, (line // 2, *halves.shape))
    sent = sent.reshape(line, row_count, heads_wide)
    along_z = exchange(jnp.concatenate((sent, peaks, docs, blank), axis=1), LINE)
    blocks = {0: along_z[:, :row_count].reshape(-1, heads_wide)}
    for step in range(1, tall // 2 + 1):
        for sign in (1, -1):
            if step < tall // 2 or sign > 0:
                hop = [(k, (k + sign) % tall) for k in range(tall)]
                blocks[-sign * step] = lax.ppermute(blocks[-sign * (step - 1)], "y", hop)
    riders = along_z[:, row_count:]
    far = lax.ppermute(near, "core", swap)
    other = jnp.concatenate(
        (jnp.where(core == 0, near, far), jnp.where(core == 0, far, near)), axis=1
    )

    even = (side == 0) & present(blocks[1]) & present(blocks[-1])
    both_rows = in_pair_order(even, normed, other)
    pair_positions = (tok_index - side) * tok_dev + jnp.arange(2 * tok_dev, dtype=jnp.int32)
    pair_positions = pair_positions.astype(jnp.float32)
    last = jnp.dot(both_rows, gathered_last, preferred_element_type=jnp.float32)
    turned = rotate(last[:, None, :], pair_positions)[:, 0]
    kept = jnp.where(side == 0, turned, last).astype(jnp.bfloat16)

    spread = to_everyone(kept, LINE).reshape(line // 2, 2, 2 * tok_dev, HEAD)
    sent_y = jnp.concatenate(
        (spread[:, 0].reshape(-1, HEAD), spread[:, 1].reshape(-1, HEAD)), axis=1
    )
    everything = lax.all_gather(sent_y, "y", axis=0, tiled=True)
    key_block, value_block = jnp.split(everything, (HEAD,), axis=1)

    peaks = jnp.max(riders[:, :peak_rows], axis=0).reshape(tall, row_count)
    ready = present(spread) & present(blocks[2]) & present(blocks[-2])
    peaks = jnp.where(ready, peaks, 0.0)
    docs = riders[:, peak_rows, :tok_dev].reshape(line * tok_dev)
    docs = jnp.broadcast_to(docs, (tall, line * tok_dev))
    arrived = exchange(jnp.concatenate((peaks, docs), axis=1), "y")
    input_peak = jnp.max(arrived[:, :row_count], axis=0).astype(jnp.float32)
    doc_block = arrived[:, row_count:].astype(jnp.int32).reshape(tok_count * tok_dev)

    block = jnp.concatenate((w_query, w_key, w_value), axis=1)
    row_peak = jnp.max(jnp.abs(block), axis=1)
    sent = jnp.concatenate(
        (
            block.reshape(tp_count, sub_rows * columns),
            jnp.broadcast_to(row_peak, (tp_count, row_count)),
        ),
        axis=1,
    )
    rows = exchange(sent, TP)
    weight_peak = jnp.max(rows[:, sub_rows * columns :], axis=0).astype(jnp.float32)
    own_rows = rows[:, : sub_rows * columns].reshape(tp_count, sub_rows, columns)

    smoothing = smooth_from(input_peak, weight_peak)
    y_index = lax.axis_index("y")
    block_rows = line * row_count
    turned = 0.0
    for offset, block_query in blocks.items():
        first = (y_index + offset) % tall * block_rows
        turned = turned + jnp.dot(
            lax.dynamic_slice_in_dim(both_rows, first, block_rows, axis=1),
            block_query,
            preferred_element_type=jnp.float32,
        )
    turned = rotate(turned.reshape(2 * tok_dev, -1, HEAD), pair_positions)
    turned = turned.astype(jnp.bfloat16).reshape(2, tok_dev, half_query)
    mine = jnp.where(side == 0, turned[0], turned[1])
    swapped = lax.ppermute(jnp.where(side == 0, turned[1], turned[0]), "pair", swap)
    query = jnp.concatenate(
        (jnp.where(side == 0, mine, swapped), jnp.where(side == 0, swapped, mine)), axis=1
    ).reshape(tok_dev, 1, group_size, HEAD)

    length = key_block.shape[0]
    scores = jnp.einsum(
        "tkgd,skd->kgts", query, key_block[:, None, :], preferred_element_type=jnp.float32
    ) * (1.0 / math.sqrt(HEAD))
    query_positions = tok_index * tok_dev + jnp.arange(tok_dev, dtype=jnp.int32)
    key_positions = jnp.arange(length, dtype=jnp.int32)
    allowed = (doc_ids[:, None] == doc_block[None, :]) & (
        key_positions[None, :] <= query_positions[:, None]
    )
    scores = jnp.where(allowed, scores, -1e30)
    highest = jnp.max(scores, axis=3, keepdims=True)
    weights = jnp.where(allowed, jnp.exp(scores - highest), 0.0)
    totals = jnp.sum(weights, axis=3)
    accumulated = jnp.einsum(
        "kgts,skd->kgtd",
        weights.astype(jnp.bfloat16),
        value_block[:, None, :],
        preferred_element_type=jnp.float32,
    )
    attended = (
        (accumulated / totals[..., None])
        .transpose(2, 0, 1, 3)
        .reshape(tok_dev, group_size * HEAD)
        .astype(jnp.bfloat16)
    )
    out_peak = jnp.max(jnp.abs(attended), axis=0).astype(jnp.float32)
    column_peak = jnp.max(jnp.abs(smoothing[:, None] * block.astype(jnp.float32)), axis=0)
    largest = jnp.concatenate((column_peak, out_peak))
    largest = jnp.max(to_everyone(largest, LINE), axis=0)
    largest = jnp.max(to_everyone(largest, "y"), axis=0)
    column_peak, out_scale = largest[:columns], largest[columns:]
    scale = jnp.maximum(column_peak, 1e-05) / 127.0
    all_scales = to_everyone(scale, TP)
    scales = jnp.split(scale, cuts)

    smooth_part = lax.dynamic_slice_in_dim(smoothing, tp_index * sub_rows, sub_rows)
    gain_part = lax.dynamic_slice_in_dim(
        norm_gain, tok_index * row_count + tp_index * sub_rows, sub_rows
    )
    folded_gain = gain_part / smooth_part
    coded = (
        smooth_part[None, :, None] * own_rows.astype(jnp.float32) / all_scales[:, None, :]
    )
    codes = tuple(
        part.transpose(1, 0, 2).reshape(sub_rows, tp_count * part.shape[2])
        for part in jnp.split(coded, cuts, axis=2)
    )

    return (
        attended,
        out_scale,
        folded_gain,
        codes[0],
        codes[1],
        codes[2],
        scales[0],
        scales[1],
        scales[2],
    )


def solution(mesh):
    split = Mesh(mesh.devices.reshape(8, 4, 2, 4, 2), ("y", "z", "pair", "x", "core"))
    placed = (P(TOK, None), P(), P(TOK, TP), P(TOK, TP), P(TOK, TP), P(TOK))
    return jax.shard_map(
        on_device,
        mesh=split,
        in_specs=placed,
        out_specs=(
            P(TOK, TP),
            P(TP),
            P(TOK_TP),
            P(TOK_TP, None),
            P(TOK_TP, None),
            P(TOK_TP, None),
            P(TP),
            P(TP),
            P(TP),
        ),
        check_vma=False,
    )
```

```python
import math

import jax
import jax.numpy as jnp
from jax import lax
from jax.sharding import Mesh
from jax.sharding import PartitionSpec as P

HEAD = 128
KVH = 8
QHEADS = 32
DOC_MOST = 4608
LINE = ("z", "pair")
TOK = ("y", "z", "pair")
TP = ("x", "core")
TOK_TP = TOK + TP


def exchange(parts, axis):
    return lax.all_to_all(parts, axis, split_axis=0, concat_axis=0, tiled=True)


def to_everyone(shard, axis):
    return exchange(jnp.broadcast_to(shard, (lax.axis_size(axis), *shard.shape)), axis)


def to_sides(even, odd):
    halves = jnp.stack((even, odd))
    sent = jnp.broadcast_to(halves, (lax.axis_size("z"), *halves.shape))
    return exchange(sent.reshape(-1, *even.shape), LINE).reshape(-1, even.shape[1])


def present(array):
    first = array.reshape(-1)[0]
    return first < 1e30


def in_pair_order(even, own, other):
    return jnp.concatenate(
        (jnp.where(even, own, other), jnp.where(even, other, own)), axis=0
    )


def rotate(states, positions):
    half = states.shape[-1] // 2
    inverse = jnp.exp(
        jnp.arange(half, dtype=jnp.float32) * (-2.0 * math.log(10000.0) / states.shape[-1])
    )
    angles = positions[:, None] * inverse[None, :]
    cosine = jnp.cos(angles)[:, None, :]
    sine = jnp.sin(angles)[:, None, :]
    first = states[..., :half]
    second = states[..., half:]
    return jnp.concatenate(
        [first * cosine - second * sine, second * cosine + first * sine], axis=-1
    )


def smooth_from(input_peak, weight_peak):
    return jnp.sqrt(jnp.maximum(input_peak, 1e-05)) / jnp.sqrt(jnp.maximum(weight_peak, 1e-05))


def on_device(hidden, norm_gain, w_query, w_key, w_value, doc_ids):
    tok_dev, width = hidden.shape
    row_count = w_query.shape[0]
    tok_count = lax.axis_size(TOK)
    tp_count = lax.axis_size(TP)
    tok_index = lax.axis_index(TOK)
    tp_index = lax.axis_index(TP)
    side = lax.axis_index("pair")
    core = lax.axis_index("core")
    line = lax.axis_size(LINE)
    tall = lax.axis_size("y")
    sub_rows = row_count // tp_count
    widths = (w_query.shape[1], w_key.shape[1], w_value.shape[1])
    cuts = (widths[0], widths[0] + widths[1])
    columns = sum(widths)
    half_query = widths[0] // 2
    group_size = QHEADS // KVH

    along_z = to_sides(w_key, w_value)
    gathered_last = lax.all_gather(along_z, "y", axis=0, tiled=True)

    states = hidden.astype(jnp.float32)
    inverse_rms = lax.rsqrt(jnp.mean(states * states, axis=1, keepdims=True) + 1e-05)
    normed = (states * inverse_rms * norm_gain[None, :]).astype(jnp.bfloat16)

    swap = [(0, 1), (1, 0)]
    channels = width // 2
    near = lax.ppermute(
        lax.dynamic_slice_in_dim(normed, core * channels, channels, axis=1), "pair", swap
    )
    heads_wide = half_query
    peaks = jnp.max(jnp.abs(normed), axis=0).reshape(tall, line, row_count)
    peaks = peaks.transpose(1, 0, 2).reshape(line, -1, heads_wide)
    docs = jnp.pad(doc_ids.astype(jnp.bfloat16), (0, heads_wide - tok_dev))
    docs = jnp.broadcast_to(docs, (line, 1, heads_wide))
    peak_rows = peaks.shape[1]
    blank = jnp.zeros((line, 15 - peak_rows, heads_wide), jnp.bfloat16)
    halves = jnp.stack((w_query[:, :half_query], w_query[:, half_query:]))
    sent = jnp.broadcast_to(halves, (line // 2, *halves.shape))
    sent = sent.reshape(line, row_count, heads_wide)
    along_z = exchange(jnp.concatenate((sent, peaks, docs, blank), axis=1), LINE)
    gathered_query = lax.all_gather(
        along_z[:, :row_count].reshape(-1, heads_wide), "y", axis=0, tiled=True
    )
    riders = along_z[:, row_count:]
    peaks = jnp.max(riders[:, :peak_rows], axis=0).reshape(tall, row_count)
    docs = riders[:, peak_rows, :tok_dev].reshape(line * tok_dev)
    docs = jnp.broadcast_to(docs, (tall, line * tok_dev))
    arrived = exchange(jnp.concatenate((peaks, docs), axis=1), "y")
    input_peak = jnp.max(arrived[:, :row_count], axis=0).astype(jnp.float32)
    doc_block = arrived[:, row_count:].astype(jnp.int32).reshape(tok_count * tok_dev)
    far = lax.ppermute(near, "core", swap)
    other = jnp.concatenate(
        (jnp.where(core == 0, near, far), jnp.where(core == 0, far, near)), axis=1
    )

    even = (side == 0) & present(along_z)
    both_rows = in_pair_order(even, normed, other)
    pair_positions = (tok_index - side) * tok_dev + jnp.arange(2 * tok_dev, dtype=jnp.int32)
    pair_positions = pair_positions.astype(jnp.float32)
    last = jnp.dot(both_rows, gathered_last, preferred_element_type=jnp.float32)
    turned = rotate(last[:, None, :], pair_positions)[:, 0]
    kept = jnp.where(side == 0, turned, last).astype(jnp.bfloat16)

    spread = to_everyone(kept, LINE).reshape(line // 2, 2, 2 * tok_dev, HEAD)
    sent_y = jnp.concatenate(
        (spread[:, 0].reshape(-1, HEAD), spread[:, 1].reshape(-1, HEAD)), axis=1
    )
    everything = lax.all_gather(sent_y, "y", axis=0, tiled=True)

    block = jnp.concatenate((w_query, w_key, w_value), axis=1)
    row_peak = jnp.max(jnp.abs(block), axis=1)
    sent = jnp.concatenate(
        (
            block.reshape(tp_count, sub_rows * columns),
            jnp.broadcast_to(row_peak, (tp_count, row_count)),
        ),
        axis=1,
    )
    rows = exchange(sent, TP)
    weight_peak = jnp.max(rows[:, sub_rows * columns :], axis=0).astype(jnp.float32)
    own_rows = rows[:, : sub_rows * columns].reshape(tp_count, sub_rows, columns)

    smoothing = smooth_from(input_peak, weight_peak)
    column_peak = jnp.max(jnp.abs(smoothing[:, None] * block.astype(jnp.float32)), axis=0)
    column_peak = jnp.where(present(spread), column_peak, 0.0)
    column_peak = jnp.max(to_everyone(column_peak, LINE), axis=0)
    column_peak = jnp.max(to_everyone(column_peak, "y"), axis=0)
    scale = jnp.maximum(column_peak, 1e-05) / 127.0
    all_scales = to_everyone(scale, TP)
    scales = jnp.split(scale, cuts)

    smooth_part = lax.dynamic_slice_in_dim(smoothing, tp_index * sub_rows, sub_rows)
    gain_part = lax.dynamic_slice_in_dim(
        norm_gain, tok_index * row_count + tp_index * sub_rows, sub_rows
    )
    folded_gain = gain_part / smooth_part
    coded = (
        smooth_part[None, :, None] * own_rows.astype(jnp.float32) / all_scales[:, None, :]
    )
    codes = tuple(
        part.transpose(1, 0, 2).reshape(sub_rows, tp_count * part.shape[2])
        for part in jnp.split(coded, cuts, axis=2)
    )

    even = (side == 0) & present(all_scales)
    both_rows = in_pair_order(even, normed, other)
    turned = jnp.dot(both_rows, gathered_query, preferred_element_type=jnp.float32)
    turned = rotate(turned.reshape(2 * tok_dev, -1, HEAD), pair_positions)
    turned = turned.astype(jnp.bfloat16).reshape(2, tok_dev, half_query)
    mine = jnp.where(side == 0, turned[0], turned[1])
    swapped = lax.ppermute(jnp.where(side == 0, turned[1], turned[0]), "pair", swap)
    query = jnp.concatenate(
        (jnp.where(side == 0, mine, swapped), jnp.where(side == 0, swapped, mine)), axis=1
    ).reshape(tok_dev, 1, group_size, HEAD)

    query_positions = tok_index * tok_dev + jnp.arange(tok_dev, dtype=jnp.int32)
    length = doc_block.shape[0]
    window = min(length, -(-(DOC_MOST - 1 + tok_dev + 127) // 256) * 256)
    start = jnp.sum((doc_block < doc_ids[0]).astype(jnp.int32)) // 128 * 128
    start = jnp.minimum(start, length - window)
    doc_window = lax.dynamic_slice_in_dim(doc_block, start, window)
    key_positions = start + jnp.arange(window, dtype=jnp.int32)
    allowed = (doc_ids[:, None] == doc_window[None, :]) & (
        key_positions[None, :] <= query_positions[:, None]
    )
    seen = lax.dynamic_slice_in_dim(everything, start, window)
    key_block, value_block = jnp.split(seen, (HEAD,), axis=1)

    scores = jnp.einsum(
        "tkgd,skd->kgts", query, key_block[:, None, :], preferred_element_type=jnp.float32
    ) * (1.0 / math.sqrt(HEAD))
    scores = jnp.where(allowed, scores, -1e30)
    highest = jnp.max(scores, axis=3, keepdims=True)
    weights = jnp.exp(scores - highest)
    totals = jnp.sum(weights, axis=3)
    accumulated = jnp.einsum(
        "kgts,skd->kgtd",
        weights.astype(jnp.bfloat16),
        value_block[:, None, :],
        preferred_element_type=jnp.float32,
    )
    attended = (
        (accumulated / totals[..., None])
        .transpose(2, 0, 1, 3)
        .reshape(tok_dev, group_size * HEAD)
        .astype(jnp.bfloat16)
    )
    out_peak = jnp.max(jnp.abs(attended), axis=0).astype(jnp.float32)
    out_scale = jnp.max(to_everyone(out_peak, TOK), axis=0)
    return (
        attended,
        out_scale,
        folded_gain,
        codes[0],
        codes[1],
        codes[2],
        scales[0],
        scales[1],
        scales[2],
    )


def solution(mesh):
    split = Mesh(mesh.devices.reshape(8, 4, 2, 4, 2), ("y", "z", "pair", "x", "core"))
    placed = (P(TOK, None), P(), P(TOK, TP), P(TOK, TP), P(TOK, TP), P(TOK))
    return jax.shard_map(
        on_device,
        mesh=split,
        in_specs=placed,
        out_specs=(
            P(TOK, TP),
            P(TP),
            P(TOK_TP),
            P(TOK_TP, None),
            P(TOK_TP, None),
            P(TOK_TP, None),
            P(TP),
            P(TP),
            P(TP),
        ),
        check_vma=False,
    )
```

```python
import math

import jax
import jax.numpy as jnp
from jax import lax
from jax.sharding import Mesh
from jax.sharding import PartitionSpec as P

HEAD = 128
KVH = 8
QHEADS = 32
LINE = ("z", "pair")
TOK = ("y", "z", "pair")
TP = ("x", "core")
TOK_TP = TOK + TP


def exchange(parts, axis):
    return lax.all_to_all(parts, axis, split_axis=0, concat_axis=0, tiled=True)


def to_everyone(shard, axis):
    return exchange(jnp.broadcast_to(shard, (lax.axis_size(axis), *shard.shape)), axis)


def by_parity(even, odd):
    receiver = lax.broadcasted_iota(jnp.int32, (lax.axis_size(LINE), 1, 1), 0)
    return jnp.where(receiver % 2 == 0, even[None], odd[None])


def to_sides(even, odd):
    return exchange(by_parity(even, odd), LINE).reshape(-1, even.shape[1])


def present(array):
    first = array.reshape(-1)[0]
    return first < 1e30


def in_pair_order(even, own, other):
    return jnp.concatenate(
        (jnp.where(even, own, other), jnp.where(even, other, own)), axis=0
    )


def rotate(states, positions):
    half = states.shape[-1] // 2
    inverse = jnp.exp(
        jnp.arange(half, dtype=jnp.float32) * (-2.0 * math.log(10000.0) / states.shape[-1])
    )
    angles = positions[:, None] * inverse[None, :]
    cosine = jnp.cos(angles)[:, None, :]
    sine = jnp.sin(angles)[:, None, :]
    first = states[..., :half]
    second = states[..., half:]
    return jnp.concatenate(
        [first * cosine - second * sine, second * cosine + first * sine], axis=-1
    )


def smooth_from(input_peak, weight_peak):
    return jnp.sqrt(jnp.maximum(input_peak, 1e-05)) / jnp.sqrt(jnp.maximum(weight_peak, 1e-05))


def on_device(hidden, norm_gain, w_query, w_key, w_value, doc_ids):
    tok_dev, width = hidden.shape
    row_count = w_query.shape[0]
    tok_count = lax.axis_size(TOK)
    tp_count = lax.axis_size(TP)
    tok_index = lax.axis_index(TOK)
    tp_index = lax.axis_index(TP)
    side = lax.axis_index("pair")
    core = lax.axis_index("core")
    line = lax.axis_size(LINE)
    tall = lax.axis_size("y")
    sub_rows = row_count // tp_count
    widths = (w_query.shape[1], w_key.shape[1], w_value.shape[1])
    cuts = (widths[0], widths[0] + widths[1])
    columns = sum(widths)
    half_query = widths[0] // 2
    group_size = QHEADS // KVH

    along_z = to_sides(w_key, w_value)
    gathered_last = lax.all_gather(along_z, "y", axis=0, tiled=True)

    states = hidden.astype(jnp.float32)
    inverse_rms = lax.rsqrt(jnp.mean(states * states, axis=1, keepdims=True) + 1e-05)
    normed = (states * inverse_rms * norm_gain[None, :]).astype(jnp.bfloat16)

    swap = [(0, 1), (1, 0)]
    channels = width // 2
    near = lax.ppermute(
        lax.dynamic_slice_in_dim(normed, core * channels, channels, axis=1), "pair", swap
    )
    heads_wide = half_query
    peaks = jnp.max(jnp.abs(normed), axis=0).reshape(tall, line, row_count)
    peaks = peaks.transpose(1, 0, 2).reshape(line, -1, heads_wide)
    docs = jnp.pad(doc_ids.astype(jnp.bfloat16), (0, heads_wide - tok_dev))
    docs = jnp.broadcast_to(docs, (line, 1, heads_wide))
    peak_rows = peaks.shape[1]
    blank = jnp.zeros((line, 15 - peak_rows, heads_wide), jnp.bfloat16)
    sent = by_parity(w_query[:, :half_query], w_query[:, half_query:])
    along_z = exchange(jnp.concatenate((sent, peaks, docs, blank), axis=1), LINE)
    gathered_query = lax.all_gather(
        along_z[:, :row_count].reshape(-1, heads_wide), "y", axis=0, tiled=True
    )
    riders = along_z[:, row_count:]
    peaks = jnp.max(riders[:, :peak_rows], axis=0).reshape(tall, row_count)
    docs = riders[:, peak_rows, :tok_dev].reshape(line * tok_dev)
    docs = jnp.broadcast_to(docs, (tall, line * tok_dev))
    arrived = exchange(jnp.concatenate((peaks, docs), axis=1), "y")
    input_peak = jnp.max(arrived[:, :row_count], axis=0).astype(jnp.float32)
    doc_block = arrived[:, row_count:].astype(jnp.int32).reshape(tok_count * tok_dev)
    far = lax.ppermute(near, "core", swap)
    other = jnp.concatenate(
        (jnp.where(core == 0, near, far), jnp.where(core == 0, far, near)), axis=1
    )

    even = (side == 0) & present(along_z)
    both_rows = in_pair_order(even, normed, other)
    pair_positions = (tok_index - side) * tok_dev + jnp.arange(2 * tok_dev, dtype=jnp.int32)
    pair_positions = pair_positions.astype(jnp.float32)
    last = jnp.dot(both_rows, gathered_last, preferred_element_type=jnp.float32)
    turned = rotate(last[:, None, :], pair_positions)[:, 0]
    kept = jnp.where(side == 0, turned, last).astype(jnp.bfloat16)

    spread = to_everyone(kept, LINE).reshape(line // 2, 2, 2 * tok_dev, HEAD)
    sent_y = jnp.concatenate(
        (spread[:, 0].reshape(-1, HEAD), spread[:, 1].reshape(-1, HEAD)), axis=1
    )
    everything = lax.all_gather(sent_y, "y", axis=0, tiled=True)
    key_block, value_block = jnp.split(everything, (HEAD,), axis=1)

    block = jnp.concatenate((w_query, w_key, w_value), axis=1)
    row_peak = jnp.max(jnp.abs(block), axis=1)
    sent = jnp.concatenate(
        (
            block.reshape(tp_count, sub_rows * columns),
            jnp.broadcast_to(row_peak, (tp_count, row_count)),
        ),
        axis=1,
    )
    rows = exchange(sent, TP)
    weight_peak = jnp.max(rows[:, sub_rows * columns :], axis=0).astype(jnp.float32)
    own_rows = rows[:, : sub_rows * columns].reshape(tp_count, sub_rows, columns)

    smoothing = smooth_from(input_peak, weight_peak)
    column_peak = jnp.max(jnp.abs(smoothing[:, None] * block.astype(jnp.float32)), axis=0)
    column_peak = jnp.where(present(spread), column_peak, 0.0)
    column_peak = jnp.max(to_everyone(column_peak, LINE), axis=0)
    column_peak = jnp.max(to_everyone(column_peak, "y"), axis=0)
    scale = jnp.maximum(column_peak, 1e-05) / 127.0
    all_scales = to_everyone(scale, TP)
    scales = jnp.split(scale, cuts)

    smooth_part = lax.dynamic_slice_in_dim(smoothing, tp_index * sub_rows, sub_rows)
    gain_part = lax.dynamic_slice_in_dim(
        norm_gain, tok_index * row_count + tp_index * sub_rows, sub_rows
    )
    folded_gain = gain_part / smooth_part
    coded = (
        smooth_part[None, :, None] * own_rows.astype(jnp.float32) / all_scales[:, None, :]
    )
    codes = tuple(
        part.transpose(1, 0, 2).reshape(sub_rows, tp_count * part.shape[2])
        for part in jnp.split(coded, cuts, axis=2)
    )

    even = (side == 0) & present(all_scales)
    both_rows = in_pair_order(even, normed, other)
    turned = jnp.dot(both_rows, gathered_query, preferred_element_type=jnp.float32)
    turned = rotate(turned.reshape(2 * tok_dev, -1, HEAD), pair_positions)
    turned = turned.astype(jnp.bfloat16).reshape(2, tok_dev, half_query)
    mine = jnp.where(side == 0, turned[0], turned[1])
    swapped = lax.ppermute(jnp.where(side == 0, turned[1], turned[0]), "pair", swap)
    query = jnp.concatenate(
        (jnp.where(side == 0, mine, swapped), jnp.where(side == 0, swapped, mine)), axis=1
    ).reshape(tok_dev, 1, group_size, HEAD)

    length = key_block.shape[0]
    scores = jnp.einsum(
        "tkgd,skd->kgts", query, key_block[:, None, :], preferred_element_type=jnp.float32
    ) * (1.0 / math.sqrt(HEAD))
    query_positions = tok_index * tok_dev + jnp.arange(tok_dev, dtype=jnp.int32)
    key_positions = jnp.arange(length, dtype=jnp.int32)
    allowed = (doc_ids[:, None] == doc_block[None, :]) & (
        key_positions[None, :] <= query_positions[:, None]
    )
    scores = jnp.where(allowed, scores, -1e30)
    highest = jnp.max(scores, axis=3, keepdims=True)
    weights = jnp.exp(scores - highest)
    totals = jnp.sum(weights, axis=3)
    accumulated = jnp.einsum(
        "kgts,skd->kgtd",
        weights.astype(jnp.bfloat16),
        value_block[:, None, :],
        preferred_element_type=jnp.float32,
    )
    attended = (
        (accumulated / totals[..., None])
        .transpose(2, 0, 1, 3)
        .reshape(tok_dev, group_size * HEAD)
        .astype(jnp.bfloat16)
    )
    out_peak = jnp.max(jnp.abs(attended), axis=0).astype(jnp.float32)
    out_scale = jnp.max(to_everyone(out_peak, TOK), axis=0)
    return (
        attended,
        out_scale,
        folded_gain,
        codes[0],
        codes[1],
        codes[2],
        scales[0],
        scales[1],
        scales[2],
    )


def solution(mesh):
    split = Mesh(mesh.devices.reshape(8, 4, 2, 4, 2), ("y", "z", "pair", "x", "core"))
    placed = (P(TOK, None), P(), P(TOK, TP), P(TOK, TP), P(TOK, TP), P(TOK))
    return jax.shard_map(
        on_device,
        mesh=split,
        in_specs=placed,
        out_specs=(
            P(TOK, TP),
            P(TP),
            P(TOK_TP),
            P(TOK_TP, None),
            P(TOK_TP, None),
            P(TOK_TP, None),
            P(TP),
            P(TP),
            P(TP),
        ),
        check_vma=False,
    )
```

```python
import math

import jax
import jax.numpy as jnp
from jax import lax
from jax.sharding import Mesh
from jax.sharding import PartitionSpec as P

HEAD = 128
KVH = 8
QHEADS = 32
LINE = ("z", "pair")
TOK = ("y", "z", "pair")
TP = ("x", "core")
TOK_TP = TOK + TP


def exchange(parts, axis):
    return lax.all_to_all(parts, axis, split_axis=0, concat_axis=0, tiled=True)


def to_everyone(shard, axis):
    return exchange(jnp.broadcast_to(shard, (lax.axis_size(axis), *shard.shape)), axis)


def by_parity(even, odd):
    receiver = lax.broadcasted_iota(jnp.int32, (lax.axis_size(LINE), 1, 1), 0)
    return jnp.where(receiver % 2 == 0, even[None], odd[None])


def to_sides(even, odd):
    return exchange(by_parity(even, odd), LINE).reshape(-1, even.shape[1])


def present(array):
    first = array.reshape(-1)[0]
    return first < 1e30


def in_pair_order(even, own, other):
    return jnp.concatenate(
        (jnp.where(even, own, other), jnp.where(even, other, own)), axis=0
    )


def rotate(states, positions):
    half = states.shape[-1] // 2
    inverse = jnp.exp(
        jnp.arange(half, dtype=jnp.float32) * (-2.0 * math.log(10000.0) / states.shape[-1])
    )
    angles = positions[:, None] * inverse[None, :]
    cosine = jnp.cos(angles)[:, None, :]
    sine = jnp.sin(angles)[:, None, :]
    first = states[..., :half]
    second = states[..., half:]
    return jnp.concatenate(
        [first * cosine - second * sine, second * cosine + first * sine], axis=-1
    )


def smooth_from(input_peak, weight_peak):
    return jnp.sqrt(jnp.maximum(input_peak, 1e-05)) / jnp.sqrt(jnp.maximum(weight_peak, 1e-05))


def on_device(hidden, norm_gain, w_query, w_key, w_value, doc_ids):
    tok_dev, width = hidden.shape
    row_count = w_query.shape[0]
    tok_count = lax.axis_size(TOK)
    tp_count = lax.axis_size(TP)
    tok_index = lax.axis_index(TOK)
    tp_index = lax.axis_index(TP)
    side = lax.axis_index("pair")
    core = lax.axis_index("core")
    line = lax.axis_size(LINE)
    tall = lax.axis_size("y")
    sub_rows = row_count // tp_count
    widths = (w_query.shape[1], w_key.shape[1], w_value.shape[1])
    cuts = (widths[0], widths[0] + widths[1])
    columns = sum(widths)
    half_query = widths[0] // 2
    group_size = QHEADS // KVH

    along_z = to_sides(w_key, w_value)
    gathered_last = lax.all_gather(along_z, "y", axis=0, tiled=True)

    states = hidden.astype(jnp.float32)
    inverse_rms = lax.rsqrt(jnp.mean(states * states, axis=1, keepdims=True) + 1e-05)
    normed = (states * inverse_rms * norm_gain[None, :]).astype(jnp.bfloat16)

    swap = [(0, 1), (1, 0)]
    channels = width // 2
    near = lax.ppermute(
        lax.dynamic_slice_in_dim(normed, core * channels, channels, axis=1), "pair", swap
    )
    heads_wide = half_query
    peaks = jnp.max(jnp.abs(normed), axis=0).reshape(tall, line, row_count)
    peaks = peaks.transpose(1, 0, 2).reshape(line, -1, heads_wide)
    docs = jnp.pad(doc_ids.astype(jnp.bfloat16), (0, heads_wide - tok_dev))
    docs = jnp.broadcast_to(docs, (line, 1, heads_wide))
    peak_rows = peaks.shape[1]
    blank = jnp.zeros((line, 15 - peak_rows, heads_wide), jnp.bfloat16)
    sent = by_parity(w_query[:, :half_query], w_query[:, half_query:])
    along_z = exchange(jnp.concatenate((sent, peaks, docs, blank), axis=1), LINE)
    gathered_query = lax.all_gather(
        along_z[:, :row_count].reshape(-1, heads_wide), "y", axis=0, tiled=True
    )
    riders = along_z[:, row_count:]
    peaks = jnp.max(riders[:, :peak_rows], axis=0).reshape(tall, row_count)
    docs = riders[:, peak_rows, :tok_dev].reshape(line * tok_dev)
    docs = jnp.broadcast_to(docs, (tall, line * tok_dev))
    arrived = exchange(jnp.concatenate((peaks, docs), axis=1), "y")
    input_peak = jnp.max(arrived[:, :row_count], axis=0).astype(jnp.float32)
    doc_block = arrived[:, row_count:].astype(jnp.int32).reshape(tok_count * tok_dev)
    far = lax.ppermute(near, "core", swap)
    other = jnp.concatenate(
        (jnp.where(core == 0, near, far), jnp.where(core == 0, far, near)), axis=1
    )

    even = (side == 0) & present(along_z)
    both_rows = in_pair_order(even, normed, other)
    pair_positions = (tok_index - side) * tok_dev + jnp.arange(2 * tok_dev, dtype=jnp.int32)
    pair_positions = pair_positions.astype(jnp.float32)
    last = jnp.dot(both_rows, gathered_last, preferred_element_type=jnp.float32)
    turned = rotate(last[:, None, :], pair_positions)[:, 0]
    kept = jnp.where(side == 0, turned, last).astype(jnp.bfloat16)

    spread = to_everyone(kept, LINE).reshape(line // 2, 2, 2 * tok_dev, HEAD)
    sent_y = jnp.concatenate(
        (spread[:, 0].reshape(-1, HEAD), spread[:, 1].reshape(-1, HEAD)), axis=1
    )
    everything = lax.all_gather(sent_y, "y", axis=0, tiled=True)
    key_block, value_block = jnp.split(everything, (HEAD,), axis=1)

    block = jnp.concatenate((w_query, w_key, w_value), axis=1)
    row_peak = jnp.max(jnp.abs(block), axis=1)
    sent = jnp.concatenate(
        (
            block.reshape(tp_count, sub_rows * columns),
            jnp.broadcast_to(row_peak, (tp_count, row_count)),
        ),
        axis=1,
    )
    rows = exchange(sent, TP)
    weight_peak = jnp.max(rows[:, sub_rows * columns :], axis=0).astype(jnp.float32)
    own_rows = rows[:, : sub_rows * columns].reshape(tp_count, sub_rows, columns)

    smoothing = smooth_from(input_peak, weight_peak)
    column_peak = jnp.max(jnp.abs(smoothing[:, None] * block.astype(jnp.float32)), axis=0)
    column_peak = jnp.where(present(spread), column_peak, 0.0)
    column_peak = jnp.max(to_everyone(column_peak, LINE), axis=0)
    column_peak = jnp.max(to_everyone(column_peak, "y"), axis=0)
    scale = jnp.maximum(column_peak, 1e-05) / 127.0
    all_scales = to_everyone(scale, TP)
    scales = jnp.split(scale, cuts)

    smooth_part = lax.dynamic_slice_in_dim(smoothing, tp_index * sub_rows, sub_rows)
    gain_part = lax.dynamic_slice_in_dim(
        norm_gain, tok_index * row_count + tp_index * sub_rows, sub_rows
    )
    folded_gain = gain_part / smooth_part
    coded = (
        smooth_part[None, :, None] * own_rows.astype(jnp.float32) / all_scales[:, None, :]
    )
    codes = tuple(
        part.transpose(1, 0, 2).reshape(sub_rows, tp_count * part.shape[2])
        for part in jnp.split(coded, cuts, axis=2)
    )

    even = (side == 0) & present(all_scales)
    both_rows = in_pair_order(even, normed, other)
    turned = jnp.dot(both_rows, gathered_query, preferred_element_type=jnp.float32)
    turned = rotate(turned.reshape(2 * tok_dev, -1, HEAD), pair_positions)
    turned = turned.astype(jnp.bfloat16).reshape(2, tok_dev, half_query)
    mine = jnp.where(side == 0, turned[0], turned[1])
    swapped = lax.ppermute(jnp.where(side == 0, turned[1], turned[0]), "pair", swap)
    query = jnp.concatenate(
        (jnp.where(side == 0, mine, swapped), jnp.where(side == 0, swapped, mine)), axis=1
    ).reshape(tok_dev, 1, group_size, HEAD)

    length = key_block.shape[0]
    scores = jnp.einsum(
        "tkgd,skd->kgts", query, key_block[:, None, :], preferred_element_type=jnp.float32
    )
    query_positions = tok_index * tok_dev + jnp.arange(tok_dev, dtype=jnp.int32)
    key_positions = jnp.arange(length, dtype=jnp.int32)
    allowed = (doc_ids[:, None] == doc_block[None, :]) & (
        key_positions[None, :] <= query_positions[:, None]
    )
    scores = jnp.where(allowed, scores, -1e30)
    highest = jnp.max(scores, axis=3, keepdims=True)
    weights = jnp.exp((scores - highest) * (1.0 / math.sqrt(HEAD)))
    totals = jnp.sum(weights, axis=3)
    accumulated = jnp.einsum(
        "kgts,skd->kgtd",
        weights.astype(jnp.bfloat16),
        value_block[:, None, :],
        preferred_element_type=jnp.float32,
    )
    attended = (
        (accumulated / totals[..., None])
        .transpose(2, 0, 1, 3)
        .reshape(tok_dev, group_size * HEAD)
        .astype(jnp.bfloat16)
    )
    out_peak = jnp.max(jnp.abs(attended), axis=0).astype(jnp.float32)
    out_scale = jnp.max(to_everyone(out_peak, TOK), axis=0)
    return (
        attended,
        out_scale,
        folded_gain,
        codes[0],
        codes[1],
        codes[2],
        scales[0],
        scales[1],
        scales[2],
    )


def solution(mesh):
    split = Mesh(mesh.devices.reshape(8, 4, 2, 4, 2), ("y", "z", "pair", "x", "core"))
    placed = (P(TOK, None), P(), P(TOK, TP), P(TOK, TP), P(TOK, TP), P(TOK))
    return jax.shard_map(
        on_device,
        mesh=split,
        in_specs=placed,
        out_specs=(
            P(TOK, TP),
            P(TP),
            P(TOK_TP),
            P(TOK_TP, None),
            P(TOK_TP, None),
            P(TOK_TP, None),
            P(TP),
            P(TP),
            P(TP),
        ),
        check_vma=False,
    )
```

```python
import math

import jax
import jax.numpy as jnp
from jax import lax
from jax.sharding import Mesh
from jax.sharding import PartitionSpec as P

HEAD = 128
KVH = 8
QHEADS = 32
LINE = ("z", "pair")
TOK = ("y", "z", "pair")
TP = ("x", "core")
TOK_TP = TOK + TP


def exchange(parts, axis):
    return lax.all_to_all(parts, axis, split_axis=0, concat_axis=0, tiled=True)


def to_everyone(shard, axis):
    return exchange(jnp.broadcast_to(shard, (lax.axis_size(axis), *shard.shape)), axis)


def by_parity(even, odd):
    receiver = lax.broadcasted_iota(jnp.int32, (lax.axis_size(LINE), 1, 1), 0)
    return jnp.where(receiver % 2 == 0, even[None], odd[None])


def to_sides(even, odd):
    return exchange(by_parity(even, odd), LINE).reshape(-1, even.shape[1])


def present(array):
    first = array.reshape(-1)[0]
    return first < 1e30


def in_pair_order(even, own, other):
    return jnp.concatenate(
        (jnp.where(even, own, other), jnp.where(even, other, own)), axis=0
    )


def rotate(states, positions):
    half = states.shape[-1] // 2
    inverse = jnp.exp(
        jnp.arange(half, dtype=jnp.float32) * (-2.0 * math.log(10000.0) / states.shape[-1])
    )
    angles = positions[:, None] * inverse[None, :]
    cosine = jnp.cos(angles)[:, None, :]
    sine = jnp.sin(angles)[:, None, :]
    first = states[..., :half]
    second = states[..., half:]
    return jnp.concatenate(
        [first * cosine - second * sine, second * cosine + first * sine], axis=-1
    )


def smooth_from(input_peak, weight_peak):
    return jnp.sqrt(jnp.maximum(input_peak, 1e-05)) / jnp.sqrt(jnp.maximum(weight_peak, 1e-05))


def on_device(hidden, norm_gain, w_query, w_key, w_value, doc_ids):
    tok_dev, width = hidden.shape
    row_count = w_query.shape[0]
    tok_count = lax.axis_size(TOK)
    tp_count = lax.axis_size(TP)
    tok_index = lax.axis_index(TOK)
    tp_index = lax.axis_index(TP)
    side = lax.axis_index("pair")
    core = lax.axis_index("core")
    line = lax.axis_size(LINE)
    tall = lax.axis_size("y")
    sub_rows = row_count // tp_count
    widths = (w_query.shape[1], w_key.shape[1], w_value.shape[1])
    cuts = (widths[0], widths[0] + widths[1])
    columns = sum(widths)
    half_query = widths[0] // 2
    group_size = QHEADS // KVH

    along_z = to_sides(w_key, w_value)
    gathered_last = lax.all_gather(along_z, "y", axis=0, tiled=True)

    states = hidden.astype(jnp.float32)
    inverse_rms = lax.rsqrt(jnp.mean(states * states, axis=1, keepdims=True) + 1e-05)
    normed = (states * inverse_rms * norm_gain[None, :]).astype(jnp.bfloat16)

    swap = [(0, 1), (1, 0)]
    channels = width // 2
    near = lax.ppermute(
        lax.dynamic_slice_in_dim(normed, core * channels, channels, axis=1), "pair", swap
    )
    heads_wide = half_query
    peaks = jnp.max(jnp.abs(normed), axis=0).reshape(tall, line, row_count)
    peaks = peaks.transpose(1, 0, 2).reshape(line, -1, heads_wide)
    docs = jnp.pad(doc_ids.astype(jnp.bfloat16), (0, heads_wide - tok_dev))
    docs = jnp.broadcast_to(docs, (line, 1, heads_wide))
    peak_rows = peaks.shape[1]
    blank = jnp.zeros((line, 15 - peak_rows, heads_wide), jnp.bfloat16)
    sent = by_parity(w_query[:, :half_query], w_query[:, half_query:])
    along_z = exchange(jnp.concatenate((sent, peaks, docs, blank), axis=1), LINE)
    gathered_query = lax.all_gather(
        along_z[:, :row_count].reshape(-1, heads_wide), "y", axis=0, tiled=True
    )
    riders = along_z[:, row_count:]
    peaks = jnp.max(riders[:, :peak_rows], axis=0).reshape(tall, row_count)
    docs = riders[:, peak_rows, :tok_dev].reshape(line * tok_dev)
    docs = jnp.broadcast_to(docs, (tall, line * tok_dev))
    arrived = exchange(jnp.concatenate((peaks, docs), axis=1), "y")
    input_peak = jnp.max(arrived[:, :row_count], axis=0).astype(jnp.float32)
    doc_block = arrived[:, row_count:].astype(jnp.int32).reshape(tok_count * tok_dev)
    far = lax.ppermute(near, "core", swap)
    other = jnp.concatenate(
        (jnp.where(core == 0, near, far), jnp.where(core == 0, far, near)), axis=1
    )

    even = (side == 0) & present(along_z)
    both_rows = in_pair_order(even, normed, other)
    pair_positions = (tok_index - side) * tok_dev + jnp.arange(2 * tok_dev, dtype=jnp.int32)
    pair_positions = pair_positions.astype(jnp.float32)
    last = jnp.dot(both_rows, gathered_last, preferred_element_type=jnp.float32)
    turned = rotate(last[:, None, :], pair_positions)[:, 0]
    kept = jnp.where(side == 0, turned, last).astype(jnp.bfloat16)

    spread = to_everyone(kept, LINE).reshape(line // 2, 2, 2 * tok_dev, HEAD)
    sent_y = jnp.concatenate(
        (spread[:, 0].reshape(-1, HEAD), spread[:, 1].reshape(-1, HEAD)), axis=1
    )
    everything = lax.all_gather(sent_y, "y", axis=0, tiled=True)
    key_block, value_block = jnp.split(everything, (HEAD,), axis=1)

    block = jnp.concatenate((w_query, w_key, w_value), axis=1)
    row_peak = jnp.max(jnp.abs(block), axis=1)
    sent = jnp.concatenate(
        (
            block.reshape(tp_count, sub_rows * columns),
            jnp.broadcast_to(row_peak, (tp_count, row_count)),
        ),
        axis=1,
    )
    rows = exchange(sent, TP)
    weight_peak = jnp.max(rows[:, sub_rows * columns :], axis=0).astype(jnp.float32)
    own_rows = rows[:, : sub_rows * columns].reshape(tp_count, sub_rows, columns)

    smoothing = smooth_from(input_peak, weight_peak)
    column_peak = jnp.max(jnp.abs(smoothing[:, None] * block.astype(jnp.float32)), axis=0)
    column_peak = jnp.where(present(spread), column_peak, 0.0)
    column_peak = jnp.max(to_everyone(column_peak, LINE), axis=0)
    column_peak = jnp.max(to_everyone(column_peak, "y"), axis=0)
    scale = jnp.maximum(column_peak, 1e-05) / 127.0
    all_scales = to_everyone(scale, TP)
    scales = jnp.split(scale, cuts)

    smooth_part = lax.dynamic_slice_in_dim(smoothing, tp_index * sub_rows, sub_rows)
    gain_part = lax.dynamic_slice_in_dim(
        norm_gain, tok_index * row_count + tp_index * sub_rows, sub_rows
    )
    folded_gain = gain_part / smooth_part
    coded = (
        smooth_part[None, :, None] * own_rows.astype(jnp.float32) / all_scales[:, None, :]
    )
    codes = tuple(
        part.transpose(1, 0, 2).reshape(sub_rows, tp_count * part.shape[2])
        for part in jnp.split(coded, cuts, axis=2)
    )

    even = (side == 0) & present(all_scales)
    both_rows = in_pair_order(even, normed, other)
    turned = jnp.dot(both_rows, gathered_query, preferred_element_type=jnp.float32)
    turned = rotate(turned.reshape(2 * tok_dev, -1, HEAD), pair_positions)
    turned = turned.astype(jnp.bfloat16).reshape(2, tok_dev, half_query)
    mine = jnp.where(side == 0, turned[0], turned[1])
    swapped = lax.ppermute(jnp.where(side == 0, turned[1], turned[0]), "pair", swap)
    query = jnp.concatenate(
        (jnp.where(side == 0, mine, swapped), jnp.where(side == 0, swapped, mine)), axis=1
    ).reshape(tok_dev, 1, group_size, HEAD)

    length = key_block.shape[0]
    scores = jnp.einsum(
        "tkgd,skd->kgts", query, key_block[:, None, :], preferred_element_type=jnp.float32
    ) * (1.0 / math.sqrt(HEAD))
    query_positions = tok_index * tok_dev + jnp.arange(tok_dev, dtype=jnp.int32)
    key_positions = jnp.arange(length, dtype=jnp.int32)
    allowed = (doc_ids[:, None] == doc_block[None, :]) & (
        key_positions[None, :] <= query_positions[:, None]
    )
    bias = lax.optimization_barrier(jnp.where(allowed, 0.0, -1e30))
    scores = scores + bias
    highest = jnp.max(scores, axis=3, keepdims=True)
    weights = jnp.exp(scores - highest)
    totals = jnp.sum(weights, axis=3)
    accumulated = jnp.einsum(
        "kgts,skd->kgtd",
        weights.astype(jnp.bfloat16),
        value_block[:, None, :],
        preferred_element_type=jnp.float32,
    )
    attended = (
        (accumulated / totals[..., None])
        .transpose(2, 0, 1, 3)
        .reshape(tok_dev, group_size * HEAD)
        .astype(jnp.bfloat16)
    )
    out_peak = jnp.max(jnp.abs(attended), axis=0).astype(jnp.float32)
    out_scale = jnp.max(to_everyone(out_peak, TOK), axis=0)
    return (
        attended,
        out_scale,
        folded_gain,
        codes[0],
        codes[1],
        codes[2],
        scales[0],
        scales[1],
        scales[2],
    )


def solution(mesh):
    split = Mesh(mesh.devices.reshape(8, 4, 2, 4, 2), ("y", "z", "pair", "x", "core"))
    placed = (P(TOK, None), P(), P(TOK, TP), P(TOK, TP), P(TOK, TP), P(TOK))
    return jax.shard_map(
        on_device,
        mesh=split,
        in_specs=placed,
        out_specs=(
            P(TOK, TP),
            P(TP),
            P(TOK_TP),
            P(TOK_TP, None),
            P(TOK_TP, None),
            P(TOK_TP, None),
            P(TP),
            P(TP),
            P(TP),
        ),
        check_vma=False,
    )
```

```python
import math

import jax
import jax.numpy as jnp
from jax import lax
from jax.sharding import Mesh
from jax.sharding import PartitionSpec as P

HEAD = 128
KVH = 8
QHEADS = 32
LINE = ("z", "pair")
TOK = ("y", "z", "pair")
TP = ("x", "core")
TOK_TP = TOK + TP


def exchange(parts, axis):
    return lax.all_to_all(parts, axis, split_axis=0, concat_axis=0, tiled=True)


def to_everyone(shard, axis):
    return exchange(jnp.broadcast_to(shard, (lax.axis_size(axis), *shard.shape)), axis)


def by_parity(even, odd):
    receiver = lax.broadcasted_iota(jnp.int32, (lax.axis_size(LINE), 1, 1), 0)
    return jnp.where(receiver % 2 == 0, even[None], odd[None])


def to_sides(even, odd):
    return exchange(by_parity(even, odd), LINE).reshape(-1, even.shape[1])


def present(array):
    first = array.reshape(-1)[0]
    return first < 1e30


def in_pair_order(even, own, other):
    return jnp.concatenate(
        (jnp.where(even, own, other), jnp.where(even, other, own)), axis=0
    )


def rotate(states, positions):
    half = states.shape[-1] // 2
    inverse = jnp.exp(
        jnp.arange(half, dtype=jnp.float32) * (-2.0 * math.log(10000.0) / states.shape[-1])
    )
    angles = positions[:, None] * inverse[None, :]
    cosine = jnp.cos(angles)[:, None, :]
    sine = jnp.sin(angles)[:, None, :]
    first = states[..., :half]
    second = states[..., half:]
    return jnp.concatenate(
        [first * cosine - second * sine, second * cosine + first * sine], axis=-1
    )


def smooth_from(input_peak, weight_peak):
    return jnp.sqrt(jnp.maximum(input_peak, 1e-05)) / jnp.sqrt(jnp.maximum(weight_peak, 1e-05))


def on_device(hidden, norm_gain, w_query, w_key, w_value, doc_ids):
    tok_dev, width = hidden.shape
    row_count = w_query.shape[0]
    tok_count = lax.axis_size(TOK)
    tp_count = lax.axis_size(TP)
    tok_index = lax.axis_index(TOK)
    tp_index = lax.axis_index(TP)
    side = lax.axis_index("pair")
    core = lax.axis_index("core")
    line = lax.axis_size(LINE)
    tall = lax.axis_size("y")
    sub_rows = row_count // tp_count
    widths = (w_query.shape[1], w_key.shape[1], w_value.shape[1])
    cuts = (widths[0], widths[0] + widths[1])
    columns = sum(widths)
    half_query = widths[0] // 2
    group_size = QHEADS // KVH

    along_z = to_sides(w_key, w_value)
    gathered_last = lax.all_gather(along_z, "y", axis=0, tiled=True)

    states = hidden.astype(jnp.float32)
    inverse_rms = lax.rsqrt(jnp.mean(states * states, axis=1, keepdims=True) + 1e-05)
    normed = (states * inverse_rms * norm_gain[None, :]).astype(jnp.bfloat16)

    swap = [(0, 1), (1, 0)]
    channels = width // 2
    near = lax.ppermute(
        lax.dynamic_slice_in_dim(normed, core * channels, channels, axis=1), "pair", swap
    )
    heads_wide = half_query
    peaks = jnp.max(jnp.abs(normed), axis=0).reshape(tall, line, row_count)
    peaks = peaks.transpose(1, 0, 2).reshape(line, -1, heads_wide)
    docs = jnp.pad(doc_ids.astype(jnp.bfloat16), (0, heads_wide - tok_dev))
    docs = jnp.broadcast_to(docs, (line, 1, heads_wide))
    peak_rows = peaks.shape[1]
    blank = jnp.zeros((line, 15 - peak_rows, heads_wide), jnp.bfloat16)
    sent = by_parity(w_query[:, :half_query], w_query[:, half_query:])
    along_z = exchange(jnp.concatenate((sent, peaks, docs, blank), axis=1), LINE)
    gathered_query = lax.all_gather(
        along_z[:, :row_count].reshape(-1, heads_wide), "y", axis=0, tiled=True
    )
    riders = along_z[:, row_count:]
    peaks = jnp.max(riders[:, :peak_rows], axis=0).reshape(tall, row_count)
    docs = riders[:, peak_rows, :tok_dev].reshape(line * tok_dev)
    docs = jnp.broadcast_to(docs, (tall, line * tok_dev))
    arrived = exchange(jnp.concatenate((peaks, docs), axis=1), "y")
    input_peak = jnp.max(arrived[:, :row_count], axis=0).astype(jnp.float32)
    doc_block = arrived[:, row_count:].astype(jnp.int32).reshape(tok_count * tok_dev)
    far = lax.ppermute(near, "core", swap)
    other = jnp.concatenate(
        (jnp.where(core == 0, near, far), jnp.where(core == 0, far, near)), axis=1
    )

    even = (side == 0) & present(along_z)
    both_rows = in_pair_order(even, normed, other)
    pair_positions = (tok_index - side) * tok_dev + jnp.arange(2 * tok_dev, dtype=jnp.int32)
    pair_positions = pair_positions.astype(jnp.float32)
    last = jnp.dot(both_rows, gathered_last, preferred_element_type=jnp.float32)
    turned = rotate(last[:, None, :], pair_positions)[:, 0]
    kept = jnp.where(side == 0, turned, last).astype(jnp.bfloat16)

    spread = to_everyone(kept, LINE).reshape(line // 2, 2, 2 * tok_dev, HEAD)
    sent_y = jnp.concatenate(
        (spread[:, 0].reshape(-1, HEAD), spread[:, 1].reshape(-1, HEAD)), axis=1
    )
    everything = lax.all_gather(sent_y, "y", axis=0, tiled=True)
    key_block, value_block = jnp.split(everything, (HEAD,), axis=1)

    block = jnp.concatenate((w_query, w_key, w_value), axis=1)
    row_peak = jnp.max(jnp.abs(block), axis=1)
    sent = jnp.concatenate(
        (
            block.reshape(tp_count, sub_rows * columns),
            jnp.broadcast_to(row_peak, (tp_count, row_count)),
        ),
        axis=1,
    )
    rows = exchange(sent, TP)
    weight_peak = jnp.max(rows[:, sub_rows * columns :], axis=0).astype(jnp.float32)
    own_rows = rows[:, : sub_rows * columns].reshape(tp_count, sub_rows, columns)

    smoothing = smooth_from(input_peak, weight_peak)
    column_peak = jnp.max(jnp.abs(smoothing[:, None] * block.astype(jnp.float32)), axis=0)
    column_peak = jnp.where(present(spread), column_peak, 0.0)
    column_peak = jnp.max(to_everyone(column_peak, LINE), axis=0)
    column_peak = jnp.max(to_everyone(column_peak, "y"), axis=0)
    scale = jnp.maximum(column_peak, 1e-05) / 127.0
    all_scales = to_everyone(scale, TP)
    scales = jnp.split(scale, cuts)

    smooth_part = lax.dynamic_slice_in_dim(smoothing, tp_index * sub_rows, sub_rows)
    gain_part = lax.dynamic_slice_in_dim(
        norm_gain, tok_index * row_count + tp_index * sub_rows, sub_rows
    )
    folded_gain = gain_part / smooth_part
    coded = (
        smooth_part[None, :, None] * own_rows.astype(jnp.float32) / all_scales[:, None, :]
    )
    codes = tuple(
        part.transpose(1, 0, 2).reshape(sub_rows, tp_count * part.shape[2])
        for part in jnp.split(coded, cuts, axis=2)
    )

    even = (side == 0) & present(all_scales)
    both_rows = in_pair_order(even, normed, other)
    turned = jnp.dot(both_rows, gathered_query, preferred_element_type=jnp.float32)
    turned = rotate(turned.reshape(2 * tok_dev, -1, HEAD), pair_positions)
    turned = turned.astype(jnp.bfloat16).reshape(2, tok_dev, half_query)
    mine = jnp.where(side == 0, turned[0], turned[1])
    swapped = lax.ppermute(jnp.where(side == 0, turned[1], turned[0]), "pair", swap)
    query = jnp.concatenate(
        (jnp.where(side == 0, mine, swapped), jnp.where(side == 0, swapped, mine)), axis=1
    ).reshape(tok_dev, 1, group_size, HEAD)

    length = key_block.shape[0]
    scores = jnp.einsum(
        "tkgd,skd->kgts", query, key_block[:, None, :], preferred_element_type=jnp.float32
    )
    query_positions = tok_index * tok_dev + jnp.arange(tok_dev, dtype=jnp.int32)
    key_positions = jnp.arange(length, dtype=jnp.int32)
    allowed = (doc_ids[:, None] == doc_block[None, :]) & (
        key_positions[None, :] <= query_positions[:, None]
    )
    bias = lax.optimization_barrier(jnp.where(allowed, 0.0, -1e30))
    scores = scores + bias
    highest = jnp.max(scores, axis=3, keepdims=True)
    weights = jnp.exp((scores - highest) * (1.0 / math.sqrt(HEAD)))
    totals = jnp.sum(weights, axis=3)
    accumulated = jnp.einsum(
        "kgts,skd->kgtd",
        weights.astype(jnp.bfloat16),
        value_block[:, None, :],
        preferred_element_type=jnp.float32,
    )
    attended = (
        (accumulated / totals[..., None])
        .transpose(2, 0, 1, 3)
        .reshape(tok_dev, group_size * HEAD)
        .astype(jnp.bfloat16)
    )
    out_peak = jnp.max(jnp.abs(attended), axis=0).astype(jnp.float32)
    out_scale = jnp.max(to_everyone(out_peak, TOK), axis=0)
    return (
        attended,
        out_scale,
        folded_gain,
        codes[0],
        codes[1],
        codes[2],
        scales[0],
        scales[1],
        scales[2],
    )


def solution(mesh):
    split = Mesh(mesh.devices.reshape(8, 4, 2, 4, 2), ("y", "z", "pair", "x", "core"))
    placed = (P(TOK, None), P(), P(TOK, TP), P(TOK, TP), P(TOK, TP), P(TOK))
    return jax.shard_map(
        on_device,
        mesh=split,
        in_specs=placed,
        out_specs=(
            P(TOK, TP),
            P(TP),
            P(TOK_TP),
            P(TOK_TP, None),
            P(TOK_TP, None),
            P(TOK_TP, None),
            P(TP),
            P(TP),
            P(TP),
        ),
        check_vma=False,
    )
```
